128 devices in a mesh: bank: 4 (over x_hi, core), lane: 32 (over z, y, x_lo).
Axes of the slice: x: 4 (x_hi: 2, x_lo: 2; x = x_hi * 2 + x_lo), y: 4, z: 4, core: 2. Of those that a mesh axis runs over, the one named last changes fastest.
Arguments:
- amplitudes: float32 [2, 1024, 128, 128], P(None, ('bank', 'lane')), may hold values from -6 to 6
- energies: float32 [1024, 128, 128], P(('bank', 'lane')), may hold values from -2 to 2
- diagonal_angles: float32 [2, 128], replicated, may hold values from 0.3 to 1.2
Outputs:
- final_parts: float32 [2, 1024, 128, 128], P(None, ('bank', 'lane'))
- marginal: float32 [256, 128, 128], P('lane', 'bank')
The draws below stay inside these ranges and needn't reach their ends.
All inputs are finite; a program needn't handle non-finite values.
Results may differ from the reference program's by a relative error of at most 0.0003.
Values sent between devices are 32-bit elements; how exact they have to be, the bound alone decides.
A program may use at most 64 MiB of HBM per device.

```python
import jax
import jax.numpy as jnp
from jax import lax

BLOCKS_DEV = 8
ROWS = 128
LANES = 128
BLOCKS = 1024
LAYERS = 2
N_BANK = 4
N_LANE = 32


def block_scale(stream_key, dims, pieces, smallest, high):
    loudness, own = 1.0, jax.random.fold_in(stream_key, 6)
    for position, blocks in pieces:
        heights = jnp.exp(jax.random.uniform(jax.random.fold_in(own, position), (blocks,), jnp.float32, smallest / len(pieces), high / len(pieces)))
        loudness = loudness * jnp.repeat(heights, dims[position] // blocks).reshape([-1 if axis == position else 1 for axis in range(len(dims))])
    return loudness


def normal_values(key, shape, width, most, shards=(), held_as=jnp.bfloat16):
    drawn = width * jax.random.normal(key, shape, jnp.float32)
    if shards:
        drawn = drawn * block_scale(key, shape, shards, -0.22, 0.18)
    return jnp.clip(drawn, -most, most).astype(held_as)


def setup_inputs(seed: int = 0) -> dict:
    splits = jax.random.split(jax.random.key(seed), 4)
    return {
        "amplitudes": normal_values(splits[0], (2, BLOCKS, ROWS, LANES), 1.0, 6.0, ((1, 128),), jnp.float32),
        "energies": jnp.clip(jax.random.uniform(splits[1], (BLOCKS, ROWS, LANES), jnp.float32, -2.0, 2.0) * block_scale(splits[1], (BLOCKS, ROWS, LANES), ((0, 128),), -0.4, 0.0), -2.0, 2.0),
        "diagonal_angles": jnp.clip(jax.random.uniform(splits[2], (LAYERS, LANES), jnp.float32, 0.3, 1.2), 0.3, 1.2),
    }


def count_bits(values, count):
    places = jnp.arange(count.bit_length() - 1, dtype=jnp.int32)
    return jnp.sum((values[..., None] >> places) & 1, axis=-1)


def walsh_table(count):
    rank = jnp.arange(count, dtype=jnp.int32)
    parity = count_bits(rank[:, None] & rank[None, :], count) % 2
    real_part = jnp.where(parity == 1, -1.0, 1.0).astype(jnp.float32) * (count ** -0.5)
    return real_part


def apply_along(values, dim):
    real_part = walsh_table(values.shape[dim])
    def times(table):
        moved = jnp.tensordot(values, table, axes=([dim], [0]), precision=lax.Precision.HIGHEST)
        return jnp.moveaxis(moved, -1, dim)
    return times(real_part)


def diagonal_step(values, levels, angle):
    turn = angle * levels
    return jnp.stack([values[0] * jnp.cos(turn) + values[1] * jnp.sin(turn), values[1] * jnp.cos(turn) - values[0] * jnp.sin(turn)])


def reference(amplitudes, energies, diagonal_angles):
    values = amplitudes
    for layer in range(LAYERS):
        values = diagonal_step(values, energies, diagonal_angles[layer])
        values = apply_along(values, 3)
        values = apply_along(values, 2)
        parts = values.reshape(2, N_BANK, N_LANE, BLOCKS_DEV, ROWS, LANES)
        parts = apply_along(parts, 1)
        parts = apply_along(parts, 2)
        parts = apply_along(parts, 3)
        values = parts.reshape(values.shape)
    chance = values[0] * values[0] + values[1] * values[1]
    marginal = jnp.mean(chance.reshape(N_BANK, -1, ROWS, LANES), axis=0)
    return values, marginal
```

```python
import jax
import jax.numpy as jnp
from jax import lax
from jax.experimental import pallas as pl
from jax.experimental.pallas import tpu as pltpu
from jax.sharding import PartitionSpec as P

LOGICAL = pl.DeviceIdType.LOGICAL
LAYER_SCALE = 2.0**-12
SIN = (
    1.0,
    -0.1666666716337204,
    0.00833333283662796,
    -0.00019841179891955107,
    2.755283276201226e-06,
    -2.493705153483461e-08,
    1.458471399207184e-10,
)
COS = (
    1.0,
    -0.5,
    0.0416666679084301,
    -0.0013888886896893382,
    2.4801460313028656e-05,
    -2.75526161885864e-07,
    2.0779600262699205e-09,
    -1.0417342335977686e-11,
)


def polynomial(coefficients, u):
    total = jnp.full_like(u, coefficients[-1] * LAYER_SCALE)
    for c in coefficients[-2::-1]:
        total = total * u + c * LAYER_SCALE
    return total


def scaled_cos_sin(turn):
    u = turn * turn
    return polynomial(COS, u), polynomial(SIN, u) * turn


def halves(x):
    high = x.astype(jnp.bfloat16)
    low = (x - high.astype(jnp.float32)).astype(jnp.bfloat16)
    return high, low


def position():
    b, l = lax.axis_index("bank"), lax.axis_index("lane")
    x = lax.div(b, 2) * 2 + lax.rem(l, 2)
    return x, lax.rem(lax.div(l, 2), 4), lax.div(l, 8), lax.rem(b, 2)


def for_peers(visit):
    x, y, z, core = position()
    across = []
    for dx in (2, 1, 3, 0):
        xx = lax.rem(x + dx, 4)
        for dc in (1, 0):
            cc = lax.rem(core + dc, 2)
            across.append((lax.div(xx, 2) * 2 + cc) * 32 + lax.rem(xx, 2))

    def plane(t, carry):
        zz = lax.rem(z + lax.div(t, 4) + 2, 4)
        yy = lax.rem(y + lax.rem(t, 4) + 2, 4)
        for a in across:
            visit(zz * 8 + yy * 2 + a)
        return carry

    lax.fori_loop(0, 10, plane, 0)
    for a in across[:-1]:
        visit(z * 8 + y * 2 + a)
    lax.fori_loop(11, 16, plane, 0)


def kernel(
    amp_ref, en_ref, angle_ref, out_ref, marg_ref,
    a, e, eb, bt, cs, b2, a2, psi, prob, half, mine, part,
    wide, tall, load_sem, e_send, e_recv, t_send, t_recv, r_send, r_recv,
    d_send, d_recv, m_send, m_recv, out_sem,
):
    bank, lane = lax.axis_index("bank"), lax.axis_index("lane")
    me = bank * 32 + lane
    core, x_hi = lax.rem(bank, 2), lax.div(bank, 2)

    barrier = pltpu.get_barrier_semaphore()
    load_e = pltpu.make_async_copy(en_ref, e, load_sem.at[0])
    load_a = pltpu.make_async_copy(amp_ref, a, load_sem.at[1])
    load_e.start()
    load_a.start()
    for_peers(lambda d: pl.semaphore_signal(barrier, inc=1, device_id=d, device_id_type=LOGICAL))

    both = lax.broadcasted_iota(jnp.int32, (128, 256), 0) & (lax.broadcasted_iota(jnp.int32, (128, 256), 1) % 128)
    for s in (4, 2, 1):
        both = both ^ (both >> s)
    wide[...] = (1 - 2 * (both & 1)).astype(jnp.float32).astype(jnp.bfloat16)
    both = lax.broadcasted_iota(jnp.int32, (256, 128), 1) & (lax.broadcasted_iota(jnp.int32, (256, 128), 0) % 128)
    for s in (4, 2, 1):
        both = both ^ (both >> s)
    tall[...] = (1 - 2 * (both & 1)).astype(jnp.float32).astype(jnp.bfloat16)

    load_e.wait()
    pl.semaphore_wait(barrier, 127)

    for_peers(
        lambda d: pltpu.make_async_remote_copy(
            src_ref=e.at[:, :, d, :],
            dst_ref=eb.at[:, pl.ds(pl.multiple_of(me * 4, 4), 4), :],
            send_sem=e_send, recv_sem=e_recv, device_id=d, device_id_type=LOGICAL,
        ).start()
    )
    load_a.wait()

    def left(re, im):
        rh, rl = halves(re)
        ih, il = halves(im)
        rhs = jnp.concatenate(
            [jnp.concatenate([rh, ih], axis=1), jnp.concatenate([rl, il], axis=1)], axis=0
        )
        got = jnp.dot(wide[...], rhs, preferred_element_type=jnp.float32)
        return got[:, :128], got[:, 128:]

    def right(block):
        return jnp.dot(
            jnp.concatenate(halves(block), axis=1), tall[...], preferred_element_type=jnp.float32
        )

    angle = angle_ref[...]

    def first(k, carry):
        blocks = []
        for q in range(2):
            c, s = scaled_cos_sin(e[q, k] * angle[0:1, :])
            re, im = a[0, q, k], a[1, q, k]
            blocks += [re * c + im * s, im * c - re * s]
        got = right(jnp.concatenate(blocks, axis=0))
        got = [got[i * 128 : (i + 1) * 128] for i in range(4)]
        for q in range(2):
            sign = 1.0 - 2.0 * q
            re, im = left(got[0] + sign * got[2], got[1] + sign * got[3])
            a[0, q, k] = re
            a[1, q, k] = im
        return carry

    lax.fori_loop(0, 4, first, 0)

    for q in range(2):
        for_peers(
            lambda d: pltpu.make_async_remote_copy(
                src_ref=a.at[:, q, :, d, :],
                dst_ref=bt.at[q, :, pl.ds(pl.multiple_of(me * 4, 4), 4), :],
                send_sem=t_send.at[q], recv_sem=t_recv.at[q], device_id=d, device_id_type=LOGICAL,
            ).start()
        )
    for q in range(2):
        for k in range(4):
            eb[q, pl.ds(me * 4 + k, 1), :] = e[q, k, pl.ds(me, 1), :]
            for i in range(2):
                bt[q, i, pl.ds(me * 4 + k, 1), :] = a[i, q, k, pl.ds(me, 1), :]

    pltpu.make_async_copy(eb.at[:, pl.ds(0, 508)], eb.at[:, pl.ds(0, 508)], e_recv).wait()

    def turns(r, carry):
        rows = pl.ds(pl.multiple_of(r * 128, 128), 128)
        for q in range(2):
            c, s = scaled_cos_sin(eb[q, rows, :] * angle[1:2, :])
            cs[q, 0, rows, :] = c
            cs[q, 1, rows, :] = s
        return carry

    lax.fori_loop(0, 4, turns, 0)

    for q in range(2):
        pltpu.make_async_copy(bt.at[q, :, pl.ds(0, 508)], bt.at[q, :, pl.ds(0, 508)], t_recv.at[q]).wait()

        def over_rows(src, dst):
            def body(r, carry):
                rows = pl.ds(pl.multiple_of(r * 128, 128), 128)
                re, im = left(src[q, 0, rows, :], src[q, 1, rows, :])
                dst[q, 0, rows, :] = re
                dst[q, 1, rows, :] = im
                return carry

            lax.fori_loop(0, 4, body, 0)

        over_rows(bt, b2)

        def middle(r, carry):
            def four(v):
                s, d, t, u = v[0] + v[1], v[0] - v[1], v[2] + v[3], v[2] - v[3]
                return [s + t, d + u, s - t, d - u]

            rows = [pl.ds(pl.multiple_of(r * 8, 8) + 128 * h, 8) for h in range(4)]
            re = four([b2[q, 0, w, :] for w in rows])
            im = four([b2[q, 1, w, :] for w in rows])
            cc = [cs[q, 0, w, :] for w in rows]
            ss = [cs[q, 1, w, :] for w in rows]
            re, im = (
                four([x * c + y * s for x, y, c, s in zip(re, im, cc, ss)]),
                four([y * c - x * s for x, y, c, s in zip(re, im, cc, ss)]),
            )
            for h in range(4):
                bt[q, 0, rows[h], :] = re[h]
                bt[q, 1, rows[h], :] = im[h]
            return carry

        lax.fori_loop(0, 16, middle, 0, unroll=4)
        over_rows(bt, b2)

        for k in range(4):
            for_peers(
                lambda d: pltpu.make_async_remote_copy(
                    src_ref=b2.at[q, :, d * 4 + k, :],
                    dst_ref=a2.at[:, q, k, me, :],
                    send_sem=r_send.at[q, k], recv_sem=r_recv.at[q, k], device_id=d, device_id_type=LOGICAL,
                ).start()
            )
        for k in range(4):
            for i in range(2):
                a2[i, q, k, pl.ds(me, 1), :] = b2[q, i, pl.ds(me * 4 + k, 1), :]

    partner = (x_hi * 2 + 1 - core) * 32 + lane
    across = ((1 - x_hi) * 2 + core) * 32 + lane

    def to_partner(k):
        return pltpu.make_async_remote_copy(
            src_ref=prob.at[k, 1 - core], dst_ref=half.at[k],
            send_sem=d_send.at[k], recv_sem=d_recv.at[k], device_id=partner, device_id_type=LOGICAL,
        )

    def to_across(k):
        return pltpu.make_async_remote_copy(
            src_ref=mine.at[k, 1 - x_hi], dst_ref=part.at[k],
            send_sem=m_send.at[k], recv_sem=m_recv.at[k], device_id=across, device_id_type=LOGICAL,
        )

    def outs(k):
        return pltpu.make_async_copy(psi.at[:, :, k], out_ref.at[:, :, k], out_sem.at[k])

    def add_partner(k):
        to_partner(k).wait_recv()
        for h in range(2):
            mine[k, h] = prob[k, core, h] + half[k, h]
        to_across(k).start()

    for k in range(4):
        for q in range(2):
            pltpu.make_async_copy(a2.at[:, q, k, pl.ds(0, 127)], a2.at[:, q, k, pl.ds(0, 127)], r_recv.at[q, k]).wait()
        blocks = []
        for q in range(2):
            sign = 1.0 - 2.0 * q
            blocks += left(a2[0, 0, k] + sign * a2[0, 1, k], a2[1, 0, k] + sign * a2[1, 1, k])
        got = right(jnp.concatenate(blocks, axis=0))
        for q in range(2):
            re, im = got[q * 256 : q * 256 + 128], got[q * 256 + 128 : q * 256 + 256]
            psi[0, q, k] = re
            psi[1, q, k] = im
            chance = re * re + im * im
            for h in range(2):
                for c in range(2):
                    at = (h * 2 + c) * 32
                    prob[k, c, h, q] = chance[at : at + 32]
        to_partner(k).start()
        outs(k).start()
        if k:
            add_partner(k - 1)
    add_partner(3)
    for k in range(4):
        to_across(k).wait_recv()
        for q in range(2):
            marg_ref[q, k] = (mine[k, x_hi, q] + part[k, q]) * 0.25
    for k in range(4):
        to_partner(k).wait_send()
        to_across(k).wait_send()
        outs(k).wait()
    pltpu.make_async_copy(eb.at[:, pl.ds(0, 508)], eb.at[:, pl.ds(0, 508)], e_send).wait()
    for q in range(2):
        pltpu.make_async_copy(bt.at[q, :, pl.ds(0, 508)], bt.at[q, :, pl.ds(0, 508)], t_send.at[q]).wait()
        for k in range(4):
            pltpu.make_async_copy(a2.at[:, q, k, pl.ds(0, 127)], a2.at[:, q, k, pl.ds(0, 127)], r_send.at[q, k]).wait()


def shards(amplitudes, energies, angles):
    f32, bf16 = jnp.float32, jnp.bfloat16
    dma = pltpu.SemaphoreType.DMA
    out, marginal = pl.pallas_call(
        kernel,
        name="walsh",
        out_shape=(
            jax.ShapeDtypeStruct((2, 2, 4, 128, 128), f32),
            jax.ShapeDtypeStruct((2, 4, 32, 128), f32),
        ),
        in_specs=[
            pl.BlockSpec(memory_space=pl.ANY),
            pl.BlockSpec(memory_space=pl.ANY),
            pl.BlockSpec(memory_space=pltpu.VMEM),
        ],
        out_specs=(pl.BlockSpec(memory_space=pl.ANY), pl.BlockSpec(memory_space=pltpu.VMEM)),
        scratch_shapes=[
            pltpu.VMEM((2, 2, 4, 128, 128), f32),
            pltpu.VMEM((2, 4, 128, 128), f32),
            pltpu.VMEM((2, 512, 128), f32),
            pltpu.VMEM((2, 2, 512, 128), f32),
            pltpu.VMEM((2, 2, 512, 128), f32),
            pltpu.VMEM((2, 2, 512, 128), f32),
            pltpu.VMEM((2, 2, 4, 128, 128), f32),
            pltpu.VMEM((2, 2, 4, 128, 128), f32),
            pltpu.VMEM((4, 2, 2, 2, 32, 128), f32),
            pltpu.VMEM((4, 2, 2, 32, 128), f32),
            pltpu.VMEM((4, 2, 2, 32, 128), f32),
            pltpu.VMEM((4, 2, 32, 128), f32),
            pltpu.VMEM((128, 256), bf16),
            pltpu.VMEM((256, 128), bf16),
            dma((2,)), dma, dma, dma((2,)), dma((2,)), dma((2, 4)), dma((2, 4)),
            dma((4,)), dma((4,)), dma((4,)), dma((4,)), dma((4,)),
        ],
        compiler_params=pltpu.CompilerParams(
            collective_id=0, has_side_effects=True, vmem_limit_bytes=48 << 20
        ),
    )(amplitudes.reshape(2, 2, 4, 128, 128), energies.reshape(2, 4, 128, 128), angles)
    return out.reshape(2, 8, 128, 128), marginal.reshape(8, 32, 128)


def solution(mesh):
    return jax.shard_map(
        shards,
        mesh=mesh,
        in_specs=(P(None, ("bank", "lane"), None, None), P(("bank", "lane"), None, None), P()),
        out_specs=(P(None, ("bank", "lane"), None, None), P("lane", "bank", None)),
        check_vma=False,
    )
```

```python
import jax
import jax.numpy as jnp
from jax import lax
from jax.experimental import pallas as pl
from jax.experimental.pallas import tpu as pltpu
from jax.sharding import PartitionSpec as P

LOGICAL = pl.DeviceIdType.LOGICAL
LAYER_SCALE = 2.0**-12
SIN = (
    1.0,
    -0.1666666716337204,
    0.00833333283662796,
    -0.00019841179891955107,
    2.755283276201226e-06,
    -2.493705153483461e-08,
    1.458471399207184e-10,
)
COS = (
    1.0,
    -0.5,
    0.0416666679084301,
    -0.0013888886896893382,
    2.4801460313028656e-05,
    -2.75526161885864e-07,
    2.0779600262699205e-09,
    -1.0417342335977686e-11,
)


def polynomial(coefficients, u):
    total = jnp.full_like(u, coefficients[-1] * LAYER_SCALE)
    for c in coefficients[-2::-1]:
        total = total * u + c * LAYER_SCALE
    return total


def scaled_cos_sin(turn):
    u = turn * turn
    return polynomial(COS, u), polynomial(SIN, u) * turn


def halves(x):
    high = x.astype(jnp.bfloat16)
    low = (x - high.astype(jnp.float32)).astype(jnp.bfloat16)
    return high, low


def position():
    b, l = lax.axis_index("bank"), lax.axis_index("lane")
    x = lax.div(b, 2) * 2 + lax.rem(l, 2)
    return x, lax.rem(lax.div(l, 2), 4), lax.div(l, 8), lax.rem(b, 2)


def for_peers(visit):
    x, y, z, core = position()
    across = []
    for dx in (2, 1, 3, 0):
        xx = lax.rem(x + dx, 4)
        for dc in (1, 0):
            cc = lax.rem(core + dc, 2)
            across.append((lax.div(xx, 2) * 2 + cc) * 32 + lax.rem(xx, 2))

    def plane(t, carry):
        zz = lax.rem(z + lax.div(t, 4) + 2, 4)
        yy = lax.rem(y + lax.rem(t, 4) + 2, 4)
        for a in across:
            visit(zz * 8 + yy * 2 + a)
        return carry

    lax.fori_loop(0, 10, plane, 0)
    for a in across[:-1]:
        visit(z * 8 + y * 2 + a)
    lax.fori_loop(11, 16, plane, 0)


def kernel(
    amp_ref, en_ref, angle_ref, out_ref, marg_ref,
    a, e, angles, eb, bt, cs, b2, a2, prob, half, mine, part,
    wide, tall, load_sem, e_send, e_recv, t_send, t_recv, r_send, r_recv,
    d_send, d_recv, m_send, m_recv,
):
    bank, lane = lax.axis_index("bank"), lax.axis_index("lane")
    me = bank * 32 + lane
    core, x_hi = lax.rem(bank, 2), lax.div(bank, 2)

    barrier = pltpu.get_barrier_semaphore()
    load_e = pltpu.make_async_copy(en_ref, e, load_sem.at[0])
    load_a = pltpu.make_async_copy(amp_ref, a, load_sem.at[1])
    load_angles = pltpu.make_async_copy(angle_ref, angles, load_sem.at[2])
    load_e.start()
    load_angles.start()
    load_a.start()
    for_peers(lambda d: pl.semaphore_signal(barrier, inc=1, device_id=d, device_id_type=LOGICAL))

    both = lax.broadcasted_iota(jnp.int32, (128, 256), 0) & (lax.broadcasted_iota(jnp.int32, (128, 256), 1) % 128)
    for s in (4, 2, 1):
        both = both ^ (both >> s)
    wide[...] = (1 - 2 * (both & 1)).astype(jnp.float32).astype(jnp.bfloat16)
    both = lax.broadcasted_iota(jnp.int32, (256, 128), 1) & (lax.broadcasted_iota(jnp.int32, (256, 128), 0) % 128)
    for s in (4, 2, 1):
        both = both ^ (both >> s)
    tall[...] = (1 - 2 * (both & 1)).astype(jnp.float32).astype(jnp.bfloat16)

    load_e.wait()
    pl.semaphore_wait(barrier, 127)

    for_peers(
        lambda d: pltpu.make_async_remote_copy(
            src_ref=e.at[:, :, d, :],
            dst_ref=eb.at[:, pl.ds(pl.multiple_of(me * 4, 4), 4), :],
            send_sem=e_send, recv_sem=e_recv, device_id=d, device_id_type=LOGICAL,
        ).start()
    )
    load_angles.wait()
    load_a.wait()

    def left(re, im):
        rh, rl = halves(re)
        ih, il = halves(im)
        rhs = jnp.concatenate(
            [jnp.concatenate([rh, ih], axis=1), jnp.concatenate([rl, il], axis=1)], axis=0
        )
        got = jnp.dot(wide[...], rhs, preferred_element_type=jnp.float32)
        return got[:, :128], got[:, 128:]

    def right(block):
        return jnp.dot(
            jnp.concatenate(halves(block), axis=1), tall[...], preferred_element_type=jnp.float32
        )

    angle = angles[...]

    def first(k, carry):
        blocks = []
        for q in range(2):
            c, s = scaled_cos_sin(e[q, k] * angle[0:1, :])
            re, im = a[0, q, k], a[1, q, k]
            blocks += [re * c + im * s, im * c - re * s]
        got = right(jnp.concatenate(blocks, axis=0))
        got = [got[i * 128 : (i + 1) * 128] for i in range(4)]
        for q in range(2):
            sign = 1.0 - 2.0 * q
            re, im = left(got[0] + sign * got[2], got[1] + sign * got[3])
            a[0, q, k] = re
            a[1, q, k] = im
        return carry

    lax.fori_loop(0, 4, first, 0)

    for q in range(2):
        for_peers(
            lambda d: pltpu.make_async_remote_copy(
                src_ref=a.at[:, q, :, d, :],
                dst_ref=bt.at[q, :, pl.ds(pl.multiple_of(me * 4, 4), 4), :],
                send_sem=t_send.at[q], recv_sem=t_recv.at[q], device_id=d, device_id_type=LOGICAL,
            ).start()
        )
    for q in range(2):
        for k in range(4):
            eb[q, pl.ds(me * 4 + k, 1), :] = e[q, k, pl.ds(me, 1), :]
            for i in range(2):
                bt[q, i, pl.ds(me * 4 + k, 1), :] = a[i, q, k, pl.ds(me, 1), :]

    pltpu.make_async_copy(eb.at[:, pl.ds(0, 508)], eb.at[:, pl.ds(0, 508)], e_recv).wait()

    def turns(r, carry):
        rows = pl.ds(pl.multiple_of(r * 128, 128), 128)
        for q in range(2):
            c, s = scaled_cos_sin(eb[q, rows, :] * angle[1:2, :])
            cs[q, 0, rows, :] = c
            cs[q, 1, rows, :] = s
        return carry

    lax.fori_loop(0, 4, turns, 0)

    for q in range(2):
        pltpu.make_async_copy(bt.at[q, :, pl.ds(0, 508)], bt.at[q, :, pl.ds(0, 508)], t_recv.at[q]).wait()

        def over_rows(src, dst):
            def body(r, carry):
                rows = pl.ds(pl.multiple_of(r * 128, 128), 128)
                re, im = left(src[q, 0, rows, :], src[q, 1, rows, :])
                dst[q, 0, rows, :] = re
                dst[q, 1, rows, :] = im
                return carry

            lax.fori_loop(0, 4, body, 0)

        over_rows(bt, b2)

        def middle(r, carry):
            def four(v):
                s, d, t, u = v[0] + v[1], v[0] - v[1], v[2] + v[3], v[2] - v[3]
                return [s + t, d + u, s - t, d - u]

            rows = [pl.ds(pl.multiple_of(r * 8, 8) + 128 * h, 8) for h in range(4)]
            re = four([b2[q, 0, w, :] for w in rows])
            im = four([b2[q, 1, w, :] for w in rows])
            cc = [cs[q, 0, w, :] for w in rows]
            ss = [cs[q, 1, w, :] for w in rows]
            re, im = (
                four([x * c + y * s for x, y, c, s in zip(re, im, cc, ss)]),
                four([y * c - x * s for x, y, c, s in zip(re, im, cc, ss)]),
            )
            for h in range(4):
                bt[q, 0, rows[h], :] = re[h]
                bt[q, 1, rows[h], :] = im[h]
            return carry

        lax.fori_loop(0, 16, middle, 0, unroll=4)
        over_rows(bt, b2)

        for k in range(4):
            for_peers(
                lambda d: pltpu.make_async_remote_copy(
                    src_ref=b2.at[q, :, d * 4 + k, :],
                    dst_ref=a2.at[:, q, k, me, :],
                    send_sem=r_send.at[q, k], recv_sem=r_recv.at[q, k], device_id=d, device_id_type=LOGICAL,
                ).start()
            )
        for k in range(4):
            for i in range(2):
                a2[i, q, k, pl.ds(me, 1), :] = b2[q, i, pl.ds(me * 4 + k, 1), :]

    partner = (x_hi * 2 + 1 - core) * 32 + lane
    across = ((1 - x_hi) * 2 + core) * 32 + lane

    def to_partner(k):
        return pltpu.make_async_remote_copy(
            src_ref=prob.at[k, 1 - core], dst_ref=half.at[k],
            send_sem=d_send.at[k], recv_sem=d_recv.at[k], device_id=partner, device_id_type=LOGICAL,
        )

    def to_across(k):
        return pltpu.make_async_remote_copy(
            src_ref=mine.at[k, 1 - x_hi], dst_ref=part.at[k],
            send_sem=m_send.at[k], recv_sem=m_recv.at[k], device_id=across, device_id_type=LOGICAL,
        )

    def add_partner(k):
        to_partner(k).wait_recv()
        for h in range(2):
            mine[k, h] = prob[k, core, h] + half[k, h]
        to_across(k).start()

    for k in range(4):
        for q in range(2):
            pltpu.make_async_copy(a2.at[:, q, k, pl.ds(0, 127)], a2.at[:, q, k, pl.ds(0, 127)], r_recv.at[q, k]).wait()
        blocks = []
        for q in range(2):
            sign = 1.0 - 2.0 * q
            blocks += left(a2[0, 0, k] + sign * a2[0, 1, k], a2[1, 0, k] + sign * a2[1, 1, k])
        got = right(jnp.concatenate(blocks, axis=0))
        for q in range(2):
            re, im = got[q * 256 : q * 256 + 128], got[q * 256 + 128 : q * 256 + 256]
            out_ref[0, q, k] = re
            out_ref[1, q, k] = im
            chance = re * re + im * im
            for h in range(2):
                for c in range(2):
                    at = (h * 2 + c) * 32
                    prob[k, c, h, q] = chance[at : at + 32]
        to_partner(k).start()
        if k:
            add_partner(k - 1)
    add_partner(3)
    for k in range(4):
        to_across(k).wait_recv()
        for q in range(2):
            marg_ref[q, k] = (mine[k, x_hi, q] + part[k, q]) * 0.25
    for k in range(4):
        to_partner(k).wait_send()
        to_across(k).wait_send()
    pltpu.make_async_copy(eb.at[:, pl.ds(0, 508)], eb.at[:, pl.ds(0, 508)], e_send).wait()
    for q in range(2):
        pltpu.make_async_copy(bt.at[q, :, pl.ds(0, 508)], bt.at[q, :, pl.ds(0, 508)], t_send.at[q]).wait()
        for k in range(4):
            pltpu.make_async_copy(a2.at[:, q, k, pl.ds(0, 127)], a2.at[:, q, k, pl.ds(0, 127)], r_send.at[q, k]).wait()


def leave(values_ref, marginal_ref, out_ref, marg_ref, sem):
    copies = [pltpu.make_async_copy(values_ref.at[i], out_ref.at[i], sem.at[i]) for i in range(2)]
    copies.append(pltpu.make_async_copy(marginal_ref, marg_ref, sem.at[2]))
    for copy in copies:
        copy.start()
    for copy in copies:
        copy.wait()


def shards(amplitudes, energies, angles):
    f32, bf16 = jnp.float32, jnp.bfloat16
    dma = pltpu.SemaphoreType.DMA
    out, marginal = pl.pallas_call(
        kernel,
        name="walsh",
        out_shape=(
            jax.ShapeDtypeStruct((2, 2, 4, 128, 128), f32),
            jax.ShapeDtypeStruct((2, 4, 32, 128), f32),
        ),
        in_specs=[
            pl.BlockSpec(memory_space=pltpu.HBM),
            pl.BlockSpec(memory_space=pltpu.HBM),
            pl.BlockSpec(memory_space=pltpu.HBM),
        ],
        out_specs=(pl.BlockSpec(memory_space=pltpu.VMEM), pl.BlockSpec(memory_space=pltpu.VMEM)),
        scratch_shapes=[
            pltpu.VMEM((2, 2, 4, 128, 128), f32),
            pltpu.VMEM((2, 4, 128, 128), f32),
            pltpu.VMEM((2, 128), f32),
            pltpu.VMEM((2, 512, 128), f32),
            pltpu.VMEM((2, 2, 512, 128), f32),
            pltpu.VMEM((2, 2, 512, 128), f32),
            pltpu.VMEM((2, 2, 512, 128), f32),
            pltpu.VMEM((2, 2, 4, 128, 128), f32),
            pltpu.VMEM((4, 2, 2, 2, 32, 128), f32),
            pltpu.VMEM((4, 2, 2, 32, 128), f32),
            pltpu.VMEM((4, 2, 2, 32, 128), f32),
            pltpu.VMEM((4, 2, 32, 128), f32),
            pltpu.VMEM((128, 256), bf16),
            pltpu.VMEM((256, 128), bf16),
            dma((3,)), dma, dma, dma((2,)), dma((2,)), dma((2, 4)), dma((2, 4)),
            dma((4,)), dma((4,)), dma((4,)), dma((4,)),
        ],
        compiler_params=pltpu.CompilerParams(
            collective_id=0, has_side_effects=True, vmem_limit_bytes=48 << 20
        ),
    )(
        pltpu.with_memory_space_constraint(amplitudes.reshape(2, 2, 4, 128, 128), pltpu.HBM),
        pltpu.with_memory_space_constraint(energies.reshape(2, 4, 128, 128), pltpu.HBM),
        pltpu.with_memory_space_constraint(angles, pltpu.HBM),
    )
    out, marginal = pl.pallas_call(
        leave,
        name="leave",
        out_shape=(
            jax.ShapeDtypeStruct(out.shape, f32),
            jax.ShapeDtypeStruct(marginal.shape, f32),
        ),
        in_specs=[pl.BlockSpec(memory_space=pltpu.VMEM)] * 2,
        out_specs=[pl.BlockSpec(memory_space=pltpu.HBM)] * 2,
        scratch_shapes=[dma((3,))],
        compiler_params=pltpu.CompilerParams(vmem_limit_bytes=8 << 20),
    )(
        pltpu.with_memory_space_constraint(out, pltpu.VMEM),
        pltpu.with_memory_space_constraint(marginal, pltpu.VMEM),
    )
    return out.reshape(2, 8, 128, 128), marginal.reshape(8, 32, 128)


def solution(mesh):
    return jax.shard_map(
        shards,
        mesh=mesh,
        in_specs=(P(None, ("bank", "lane"), None, None), P(("bank", "lane"), None, None), P()),
        out_specs=(P(None, ("bank", "lane"), None, None), P("lane", "bank", None)),
        check_vma=False,
    )
```

```python
import collections
import itertools

import jax
import jax.numpy as jnp
from jax import lax
from jax.experimental import pallas as pl
from jax.experimental.pallas import tpu as pltpu
from jax.sharding import PartitionSpec as P

LOGICAL = pl.DeviceIdType.LOGICAL
LAYER_SCALE = 2.0**-12
SIN = (
    1.0,
    -0.1666666716337204,
    0.00833333283662796,
    -0.00019841179891955107,
    2.755283276201226e-06,
    -2.493705153483461e-08,
    1.458471399207184e-10,
)
COS = (
    1.0,
    -0.5,
    0.0416666679084301,
    -0.0013888886896893382,
    2.4801460313028656e-05,
    -2.75526161885864e-07,
    2.0779600262699205e-09,
    -1.0417342335977686e-11,
)


def polynomial(coefficients, u):
    total = jnp.full_like(u, coefficients[-1] * LAYER_SCALE)
    for c in coefficients[-2::-1]:
        total = total * u + c * LAYER_SCALE
    return total


def scaled_cos_sin(turn):
    u = turn * turn
    return polynomial(COS, u), polynomial(SIN, u) * turn


def halves(x):
    high = x.astype(jnp.bfloat16)
    low = (x - high.astype(jnp.float32)).astype(jnp.bfloat16)
    return high, low


def position():
    b, l = lax.axis_index("bank"), lax.axis_index("lane")
    x = lax.div(b, 2) * 2 + lax.rem(l, 2)
    return x, lax.rem(lax.div(l, 2), 4), lax.div(l, 8), lax.rem(b, 2)


def hops(d):
    return min(d, 4 - d)


def peer_offsets():
    todo = [o for o in itertools.product(range(4), range(4), range(4), range(2)) if any(o)]
    links = lambda ax, d: [(ax, 1)] if d == 1 else [(ax, -1)] if d == 3 else [(ax, 1), (ax, -1)]
    load, order = collections.Counter(), []
    while todo:
        far = max(sum(map(hops, o[:3])) for o in todo)

        def cost(o):
            uses = [links(ax, d) for ax, d in enumerate(o[:3]) if d]
            return sum(sum(load[u] for u in use) / len(use) for use in uses)

        best = min((o for o in todo if sum(map(hops, o[:3])) == far), key=cost)
        todo.remove(best)
        order.append(best)
        for ax, d in enumerate(best[:3]):
            if d:
                for use in links(ax, d):
                    load[use] += hops(d) / len(links(ax, d))
    return order


OFFSETS = peer_offsets()


def peers():
    x, y, z, core = position()
    xs = {}
    for dx, dc in itertools.product(range(4), range(2)):
        xx, cc = lax.rem(x + dx, 4), lax.rem(core + dc, 2)
        xs[dx, dc] = (lax.div(xx, 2) * 2 + cc) * 32 + lax.rem(xx, 2)
    ys = [lax.rem(y + d, 4) * 2 for d in range(4)]
    zs = [lax.rem(z + d, 4) * 8 for d in range(4)]
    return xs, ys, zs


def for_peers(numbers, visit):
    xs, ys, zs = numbers
    for dx, dy, dz, dc in OFFSETS:
        visit(xs[dx, dc] + (ys[dy] + zs[dz]))


STEPS = 4


def slice_of(q, step):
    width = 4 // STEPS if q else 4
    return list(range(step * width, (step + 1) * width))


def kernel(
    amp_ref, en_ref, angle_ref, out_ref, marg_ref,
    a, e, angles, eb, bt, cs, b2, a2, prob, half, mine, part, last,
    wide, tall, load_sem, e_send, e_recv, t_send, t_recv, r_send, r_recv,
    d_send, d_recv, m_send, m_recv, l_send, l_recv,
):
    bank, lane = lax.axis_index("bank"), lax.axis_index("lane")
    me = bank * 32 + lane
    core, x_hi = lax.rem(bank, 2), lax.div(bank, 2)

    numbers = peers()
    barrier = pltpu.get_barrier_semaphore()
    load_e = pltpu.make_async_copy(en_ref, e, load_sem.at[0])
    load_a = pltpu.make_async_copy(amp_ref, a, load_sem.at[1])
    load_angles = pltpu.make_async_copy(angle_ref, angles, load_sem.at[2])
    load_e.start()
    load_angles.start()
    load_a.start()
    for_peers(numbers, lambda d: pl.semaphore_signal(barrier, inc=1, device_id=d, device_id_type=LOGICAL))

    both = lax.broadcasted_iota(jnp.int32, (128, 256), 0) & (lax.broadcasted_iota(jnp.int32, (128, 256), 1) % 128)
    for s in (4, 2, 1):
        both = both ^ (both >> s)
    wide[...] = (1 - 2 * (both & 1)).astype(jnp.float32).astype(jnp.bfloat16)
    both = lax.broadcasted_iota(jnp.int32, (256, 128), 1) & (lax.broadcasted_iota(jnp.int32, (256, 128), 0) % 128)
    for s in (4, 2, 1):
        both = both ^ (both >> s)
    tall[...] = (1 - 2 * (both & 1)).astype(jnp.float32).astype(jnp.bfloat16)

    load_e.wait()
    pl.semaphore_wait(barrier, 127)

    def send_energies(q):
        for_peers(
            numbers,
            lambda d: pltpu.make_async_remote_copy(
                src_ref=e.at[q, :, d, :],
                dst_ref=eb.at[q, pl.ds(pl.multiple_of(me * 4, 4), 4), :],
                send_sem=e_send.at[q], recv_sem=e_recv.at[q], device_id=d, device_id_type=LOGICAL,
            ).start()
        )

    def energies_done(q, sem):
        rows = eb.at[q, pl.ds(0, 508)]
        return pltpu.make_async_copy(rows, rows, sem.at[q])

    send_energies(0)
    load_angles.wait()
    load_a.wait()

    def left(re, im):
        rh, rl = halves(re)
        ih, il = halves(im)
        rhs = jnp.concatenate(
            [jnp.concatenate([rh, ih], axis=1), jnp.concatenate([rl, il], axis=1)], axis=0
        )
        got = jnp.dot(wide[...], rhs, preferred_element_type=jnp.float32)
        return got[:, :128], got[:, 128:]

    def right(block):
        return jnp.dot(
            jnp.concatenate(halves(block), axis=1), tall[...], preferred_element_type=jnp.float32
        )

    angle = angles[...]

    def first(k, carry):
        blocks = []
        for q in range(2):
            c, s = scaled_cos_sin(e[q, k] * angle[0:1, :])
            re, im = a[0, q, k], a[1, q, k]
            blocks += [re * c + im * s, im * c - re * s]
        got = right(jnp.concatenate(blocks, axis=0))
        got = [got[i * 128 : (i + 1) * 128] for i in range(4)]
        for q in range(2):
            sign = 1.0 - 2.0 * q
            re, im = left(got[0] + sign * got[2], got[1] + sign * got[3])
            a[0, q, k] = re
            a[1, q, k] = im
        return carry

    lax.fori_loop(0, 4, first, 0)

    for q in range(2):
        if q:
            send_energies(1)
        for_peers(
            numbers,
            lambda d: pltpu.make_async_remote_copy(
                src_ref=a.at[:, q, :, d, :],
                dst_ref=bt.at[q, :, pl.ds(pl.multiple_of(me * 4, 4), 4), :],
                send_sem=t_send.at[q], recv_sem=t_recv.at[q], device_id=d, device_id_type=LOGICAL,
            ).start()
        )
    for q in range(2):
        for k in range(4):
            eb[q, pl.ds(me * 4 + k, 1), :] = e[q, k, pl.ds(me, 1), :]
            for i in range(2):
                bt[q, i, pl.ds(me * 4 + k, 1), :] = a[i, q, k, pl.ds(me, 1), :]

    for q in range(2):
        energies_done(q, e_recv).wait()

        def turns(r, carry):
            rows = pl.ds(pl.multiple_of(r * 64, 64), 64)
            c, s = scaled_cos_sin(eb[q, rows, :] * angle[1:2, :])
            cs[q, 0, rows, :] = c
            cs[q, 1, rows, :] = s
            return carry

        lax.fori_loop(0, 8, turns, 0)
        pltpu.make_async_copy(bt.at[q, :, pl.ds(0, 508)], bt.at[q, :, pl.ds(0, 508)], t_recv.at[q]).wait()

        def over_rows(src, dst):
            for r in range(4):
                rows = slice(r * 128, (r + 1) * 128)
                re, im = left(src[q, 0, rows, :], src[q, 1, rows, :])
                dst[q, 0, rows, :] = re
                dst[q, 1, rows, :] = im

        over_rows(bt, b2)

        def middle(r, carry):
            def four(v):
                s, d, t, u = v[0] + v[1], v[0] - v[1], v[2] + v[3], v[2] - v[3]
                return [s + t, d + u, s - t, d - u]

            rows = [pl.ds(pl.multiple_of(r * 8, 8) + 128 * h, 8) for h in range(4)]
            re = four([b2[q, 0, w, :] for w in rows])
            im = four([b2[q, 1, w, :] for w in rows])
            cc = [cs[q, 0, w, :] for w in rows]
            ss = [cs[q, 1, w, :] for w in rows]
            re, im = (
                four([x * c + y * s for x, y, c, s in zip(re, im, cc, ss)]),
                four([y * c - x * s for x, y, c, s in zip(re, im, cc, ss)]),
            )
            for h in range(4):
                bt[q, 0, rows[h], :] = re[h]
                bt[q, 1, rows[h], :] = im[h]
            return carry

        lax.fori_loop(0, 16, middle, 0, unroll=4)
        over_rows(bt, b2)

        for step in range(STEPS if q else 1):
            ks = slice_of(q, step)
            for_peers(
                numbers,
                lambda d: pltpu.make_async_remote_copy(
                    src_ref=b2.at[q, :, pl.ds(d * 4 + ks[0], len(ks)), :],
                    dst_ref=a2.at[:, q, ks[0] : ks[0] + len(ks), me, :],
                    send_sem=r_send.at[q, step], recv_sem=r_recv.at[q, step], device_id=d, device_id_type=LOGICAL,
                ).start()
            )
        for k in range(4):
            for i in range(2):
                a2[i, q, k, pl.ds(me, 1), :] = b2[q, i, pl.ds(me * 4 + k, 1), :]

    def returned(q, step, sem):
        ks = slice_of(q, step)
        rows = a2.at[:, q, ks[0] : ks[0] + len(ks), pl.ds(0, 127)]
        return pltpu.make_async_copy(rows, rows, sem.at[q, step])

    partner = (x_hi * 2 + 1 - core) * 32 + lane
    across = ((1 - x_hi) * 2 + core) * 32 + lane

    def to_partner(k):
        return pltpu.make_async_remote_copy(
            src_ref=prob.at[k, 1 - core], dst_ref=half.at[k],
            send_sem=d_send.at[k], recv_sem=d_recv.at[k], device_id=partner, device_id_type=LOGICAL,
        )

    def to_across(k):
        return pltpu.make_async_remote_copy(
            src_ref=mine.at[k, 1 - x_hi], dst_ref=part.at[k],
            send_sem=m_send.at[k], recv_sem=m_recv.at[k], device_id=across, device_id_type=LOGICAL,
        )

    def direct(other):
        c = lax.rem(core + other, 2)
        h = lax.rem(x_hi + other // 2, 2)
        return pltpu.make_async_remote_copy(
            src_ref=prob.at[3, c, h], dst_ref=last.at[other - 1],
            send_sem=l_send.at[other - 1], recv_sem=l_recv.at[other - 1],
            device_id=(h * 2 + c) * 32 + lane, device_id_type=LOGICAL,
        )

    def add_partner(k):
        to_partner(k).wait_recv()
        for h in range(2):
            mine[k, h] = prob[k, core, h] + half[k, h]
        to_across(k).start()

    for k in range(4):
        if k == 0:
            returned(0, 0, r_recv).wait()
        if k % (4 // STEPS) == 0:
            returned(1, k // (4 // STEPS), r_recv).wait()
        blocks = []
        for q in range(2):
            sign = 1.0 - 2.0 * q
            blocks += left(a2[0, 0, k] + sign * a2[0, 1, k], a2[1, 0, k] + sign * a2[1, 1, k])
        got = right(jnp.concatenate(blocks, axis=0))
        for q in range(2):
            re, im = got[q * 256 : q * 256 + 128], got[q * 256 + 128 : q * 256 + 256]
            out_ref[0, q, k] = re
            out_ref[1, q, k] = im
            chance = re * re + im * im
            for h in range(2):
                for c in range(2):
                    at = (h * 2 + c) * 32
                    prob[k, c, h, q] = chance[at : at + 32]
        if k < 3:
            to_partner(k).start()
        else:
            for other in (2, 3, 1):
                direct(other).start()
        if k:
            add_partner(k - 1)
    for k in range(3):
        to_across(k).wait_recv()
        for q in range(2):
            marg_ref[q, k] = (mine[k, x_hi, q] + part[k, q]) * 0.25
    for other in (1, 2, 3):
        direct(other).wait_recv()
    for q in range(2):
        marg_ref[q, 3] = ((prob[3, core, x_hi, q] + last[0, q]) + (last[1, q] + last[2, q])) * 0.25
    for k in range(3):
        to_partner(k).wait_send()
        to_across(k).wait_send()
        direct(k + 1).wait_send()
    for q in range(2):
        energies_done(q, e_send).wait()
        pltpu.make_async_copy(bt.at[q, :, pl.ds(0, 508)], bt.at[q, :, pl.ds(0, 508)], t_send.at[q]).wait()
        for step in range(STEPS if q else 1):
            returned(q, step, r_send).wait()


def leave(values_ref, marginal_ref, out_ref, marg_ref, sem):
    copies = [pltpu.make_async_copy(values_ref.at[i], out_ref.at[i], sem.at[i]) for i in range(2)]
    copies.append(pltpu.make_async_copy(marginal_ref, marg_ref, sem.at[2]))
    for copy in copies:
        copy.start()
    for copy in copies:
        copy.wait()


def shards(amplitudes, energies, angles):
    f32, bf16 = jnp.float32, jnp.bfloat16
    dma = pltpu.SemaphoreType.DMA
    out, marginal = pl.pallas_call(
        kernel,
        name="walsh",
        out_shape=(
            jax.ShapeDtypeStruct((2, 2, 4, 128, 128), f32),
            jax.ShapeDtypeStruct((2, 4, 32, 128), f32),
        ),
        in_specs=[
            pl.BlockSpec(memory_space=pltpu.HBM),
            pl.BlockSpec(memory_space=pltpu.HBM),
            pl.BlockSpec(memory_space=pltpu.HBM),
        ],
        out_specs=(pl.BlockSpec(memory_space=pltpu.VMEM), pl.BlockSpec(memory_space=pltpu.VMEM)),
        scratch_shapes=[
            pltpu.VMEM((2, 2, 4, 128, 128), f32),
            pltpu.VMEM((2, 4, 128, 128), f32),
            pltpu.VMEM((2, 128), f32),
            pltpu.VMEM((2, 512, 128), f32),
            pltpu.VMEM((2, 2, 512, 128), f32),
            pltpu.VMEM((2, 2, 512, 128), f32),
            pltpu.VMEM((2, 2, 512, 128), f32),
            pltpu.VMEM((2, 2, 4, 128, 128), f32),
            pltpu.VMEM((4, 2, 2, 2, 32, 128), f32),
            pltpu.VMEM((3, 2, 2, 32, 128), f32),
            pltpu.VMEM((3, 2, 2, 32, 128), f32),
            pltpu.VMEM((3, 2, 32, 128), f32),
            pltpu.VMEM((3, 2, 32, 128), f32),
            pltpu.VMEM((128, 256), bf16),
            pltpu.VMEM((256, 128), bf16),
            dma((3,)), dma((2,)), dma((2,)), dma((2,)), dma((2,)), dma((2, 4)), dma((2, 4)),
            dma((3,)), dma((3,)), dma((3,)), dma((3,)), dma((3,)), dma((3,)),
        ],
        compiler_params=pltpu.CompilerParams(
            collective_id=0, has_side_effects=True, vmem_limit_bytes=48 << 20
        ),
    )(
        pltpu.with_memory_space_constraint(amplitudes.reshape(2, 2, 4, 128, 128), pltpu.HBM),
        pltpu.with_memory_space_constraint(energies.reshape(2, 4, 128, 128), pltpu.HBM),
        pltpu.with_memory_space_constraint(angles, pltpu.HBM),
    )
    out, marginal = pl.pallas_call(
        leave,
        name="leave",
        out_shape=(
            jax.ShapeDtypeStruct(out.shape, f32),
            jax.ShapeDtypeStruct(marginal.shape, f32),
        ),
        in_specs=[pl.BlockSpec(memory_space=pltpu.VMEM)] * 2,
        out_specs=[pl.BlockSpec(memory_space=pltpu.HBM)] * 2,
        scratch_shapes=[dma((3,))],
        compiler_params=pltpu.CompilerParams(vmem_limit_bytes=8 << 20),
    )(
        pltpu.with_memory_space_constraint(out, pltpu.VMEM),
        pltpu.with_memory_space_constraint(marginal, pltpu.VMEM),
    )
    return out.reshape(2, 8, 128, 128), marginal.reshape(8, 32, 128)


def solution(mesh):
    return jax.shard_map(
        shards,
        mesh=mesh,
        in_specs=(P(None, ("bank", "lane"), None, None), P(("bank", "lane"), None, None), P()),
        out_specs=(P(None, ("bank", "lane"), None, None), P("lane", "bank", None)),
        check_vma=False,
    )
```

```python
import collections
import itertools

import jax
import jax.numpy as jnp
from jax import lax
from jax.experimental import pallas as pl
from jax.experimental.pallas import tpu as pltpu
from jax.sharding import PartitionSpec as P

LOGICAL = pl.DeviceIdType.LOGICAL
LAYER_SCALE = 2.0**-12
SIN = (
    1.0,
    -0.1666666716337204,
    0.00833333283662796,
    -0.00019841179891955107,
    2.755283276201226e-06,
    -2.493705153483461e-08,
    1.458471399207184e-10,
)
COS = (
    1.0,
    -0.5,
    0.0416666679084301,
    -0.0013888886896893382,
    2.4801460313028656e-05,
    -2.75526161885864e-07,
    2.0779600262699205e-09,
    -1.0417342335977686e-11,
)


def polynomial(coefficients, u):
    total = jnp.full_like(u, coefficients[-1] * LAYER_SCALE)
    for c in coefficients[-2::-1]:
        total = total * u + c * LAYER_SCALE
    return total


def scaled_cos_sin(turn):
    u = turn * turn
    return polynomial(COS, u), polynomial(SIN, u) * turn


def halves(x):
    high = x.astype(jnp.bfloat16)
    low = (x - high.astype(jnp.float32)).astype(jnp.bfloat16)
    return high, low


def position():
    b, l = lax.axis_index("bank"), lax.axis_index("lane")
    x = lax.div(b, 2) * 2 + lax.rem(l, 2)
    return x, lax.rem(lax.div(l, 2), 4), lax.div(l, 8), lax.rem(b, 2)


def hops(d):
    return min(d, 4 - d)


def peer_offsets():
    todo = [o for o in itertools.product(range(4), range(4), range(4), range(2)) if any(o)]
    links = lambda ax, d: [(ax, 1)] if d == 1 else [(ax, -1)] if d == 3 else [(ax, 1), (ax, -1)]
    load, order = collections.Counter(), []
    while todo:
        far = max(sum(map(hops, o[:3])) for o in todo)

        def cost(o):
            uses = [links(ax, d) for ax, d in enumerate(o[:3]) if d]
            return sum(sum(load[u] for u in use) / len(use) for use in uses)

        best = min((o for o in todo if sum(map(hops, o[:3])) == far), key=cost)
        todo.remove(best)
        order.append(best)
        for ax, d in enumerate(best[:3]):
            if d:
                for use in links(ax, d):
                    load[use] += hops(d) / len(links(ax, d))
    return order


OFFSETS = peer_offsets()


def peers():
    x, y, z, core = position()
    xs = {}
    for dx, dc in itertools.product(range(4), range(2)):
        xx, cc = lax.rem(x + dx, 4), lax.rem(core + dc, 2)
        xs[dx, dc] = (lax.div(xx, 2) * 2 + cc) * 32 + lax.rem(xx, 2)
    ys = [lax.rem(y + d, 4) * 2 for d in range(4)]
    zs = [lax.rem(z + d, 4) * 8 for d in range(4)]
    return xs, ys, zs


def for_peers(numbers, visit):
    xs, ys, zs = numbers
    for dx, dy, dz, dc in OFFSETS:
        visit(xs[dx, dc] + (ys[dy] + zs[dz]))


STEPS = 4


def slice_of(q, step):
    width = 4 // STEPS if q else 4
    return list(range(step * width, (step + 1) * width))


def kernel(
    amp_ref, en_ref, angle_ref, out_ref, marg_ref,
    a, e, angles, eb, bt, cs, b2, a2, prob, half, mine, part, last,
    wide, tall, load_sem, e_send, e_recv, t_send, t_recv, r_send, r_recv,
    d_send, d_recv, m_send, m_recv, l_send, l_recv,
):
    bank, lane = lax.axis_index("bank"), lax.axis_index("lane")
    me = bank * 32 + lane
    core, x_hi = lax.rem(bank, 2), lax.div(bank, 2)

    numbers = peers()
    barrier = pltpu.get_barrier_semaphore()
    load_e = pltpu.make_async_copy(en_ref, e, load_sem.at[0])
    load_a = pltpu.make_async_copy(amp_ref, a, load_sem.at[1])
    load_angles = pltpu.make_async_copy(angle_ref, angles, load_sem.at[2])
    load_e.start()
    load_angles.start()
    load_a.start()
    for_peers(numbers, lambda d: pl.semaphore_signal(barrier, inc=1, device_id=d, device_id_type=LOGICAL))

    both = lax.broadcasted_iota(jnp.int32, (128, 256), 0) & (lax.broadcasted_iota(jnp.int32, (128, 256), 1) % 128)
    for s in (4, 2, 1):
        both = both ^ (both >> s)
    wide[...] = (1 - 2 * (both & 1)).astype(jnp.float32).astype(jnp.bfloat16)
    both = lax.broadcasted_iota(jnp.int32, (256, 128), 1) & (lax.broadcasted_iota(jnp.int32, (256, 128), 0) % 128)
    for s in (4, 2, 1):
        both = both ^ (both >> s)
    tall[...] = (1 - 2 * (both & 1)).astype(jnp.float32).astype(jnp.bfloat16)


    def send_energies(q):
        for_peers(
            numbers,
            lambda d: pltpu.make_async_remote_copy(
                src_ref=e.at[q, :, d, :],
                dst_ref=eb.at[q, pl.ds(pl.multiple_of(me * 4, 4), 4), :],
                send_sem=e_send.at[q], recv_sem=e_recv.at[q], device_id=d, device_id_type=LOGICAL,
            ).start()
        )

    def energies_done(q, sem):
        rows = eb.at[q, pl.ds(0, 508)]
        return pltpu.make_async_copy(rows, rows, sem.at[q])

    load_e.wait()
    load_angles.wait()
    load_a.wait()

    def left(re, im):
        rh, rl = halves(re)
        ih, il = halves(im)
        rhs = jnp.concatenate(
            [jnp.concatenate([rh, ih], axis=1), jnp.concatenate([rl, il], axis=1)], axis=0
        )
        got = jnp.dot(wide[...], rhs, preferred_element_type=jnp.float32)
        return got[:, :128], got[:, 128:]

    def right(block):
        return jnp.dot(
            jnp.concatenate(halves(block), axis=1), tall[...], preferred_element_type=jnp.float32
        )

    angle = angles[...]

    def first(k, carry):
        blocks = []
        for q in range(2):
            c, s = scaled_cos_sin(e[q, k] * angle[0:1, :])
            re, im = a[0, q, k], a[1, q, k]
            blocks += [re * c + im * s, im * c - re * s]
        got = right(jnp.concatenate(blocks, axis=0))
        got = [got[i * 128 : (i + 1) * 128] for i in range(4)]
        for q in range(2):
            sign = 1.0 - 2.0 * q
            re, im = left(got[0] + sign * got[2], got[1] + sign * got[3])
            a[0, q, k] = re
            a[1, q, k] = im
        return carry

    lax.fori_loop(0, 4, first, 0)
    pl.semaphore_wait(barrier, 127)

    for q in range(2):
        send_energies(q)
        for_peers(
            numbers,
            lambda d: pltpu.make_async_remote_copy(
                src_ref=a.at[:, q, :, d, :],
                dst_ref=bt.at[q, :, pl.ds(pl.multiple_of(me * 4, 4), 4), :],
                send_sem=t_send.at[q], recv_sem=t_recv.at[q], device_id=d, device_id_type=LOGICAL,
            ).start()
        )
    for q in range(2):
        for k in range(4):
            eb[q, pl.ds(me * 4 + k, 1), :] = e[q, k, pl.ds(me, 1), :]
            for i in range(2):
                bt[q, i, pl.ds(me * 4 + k, 1), :] = a[i, q, k, pl.ds(me, 1), :]

    for q in range(2):
        energies_done(q, e_recv).wait()

        def turns(r, carry):
            rows = pl.ds(pl.multiple_of(r * 64, 64), 64)
            c, s = scaled_cos_sin(eb[q, rows, :] * angle[1:2, :])
            cs[q, 0, rows, :] = c
            cs[q, 1, rows, :] = s
            return carry

        lax.fori_loop(0, 8, turns, 0)
        pltpu.make_async_copy(bt.at[q, :, pl.ds(0, 508)], bt.at[q, :, pl.ds(0, 508)], t_recv.at[q]).wait()

        def over_rows(src, dst):
            for r in range(4):
                rows = slice(r * 128, (r + 1) * 128)
                re, im = left(src[q, 0, rows, :], src[q, 1, rows, :])
                dst[q, 0, rows, :] = re
                dst[q, 1, rows, :] = im

        over_rows(bt, b2)

        def middle(r, carry):
            def four(v):
                s, d, t, u = v[0] + v[1], v[0] - v[1], v[2] + v[3], v[2] - v[3]
                return [s + t, d + u, s - t, d - u]

            rows = [pl.ds(pl.multiple_of(r * 8, 8) + 128 * h, 8) for h in range(4)]
            re = four([b2[q, 0, w, :] for w in rows])
            im = four([b2[q, 1, w, :] for w in rows])
            cc = [cs[q, 0, w, :] for w in rows]
            ss = [cs[q, 1, w, :] for w in rows]
            re, im = (
                four([x * c + y * s for x, y, c, s in zip(re, im, cc, ss)]),
                four([y * c - x * s for x, y, c, s in zip(re, im, cc, ss)]),
            )
            for h in range(4):
                bt[q, 0, rows[h], :] = re[h]
                bt[q, 1, rows[h], :] = im[h]
            return carry

        lax.fori_loop(0, 16, middle, 0, unroll=4)
        over_rows(bt, b2)

        for step in range(STEPS if q else 1):
            ks = slice_of(q, step)
            for_peers(
                numbers,
                lambda d: pltpu.make_async_remote_copy(
                    src_ref=b2.at[q, :, pl.ds(d * 4 + ks[0], len(ks)), :],
                    dst_ref=a2.at[:, q, ks[0] : ks[0] + len(ks), me, :],
                    send_sem=r_send.at[q, step], recv_sem=r_recv.at[q, step], device_id=d, device_id_type=LOGICAL,
                ).start()
            )
        for k in range(4):
            for i in range(2):
                a2[i, q, k, pl.ds(me, 1), :] = b2[q, i, pl.ds(me * 4 + k, 1), :]

    def returned(q, step, sem):
        ks = slice_of(q, step)
        rows = a2.at[:, q, ks[0] : ks[0] + len(ks), pl.ds(0, 127)]
        return pltpu.make_async_copy(rows, rows, sem.at[q, step])

    partner = (x_hi * 2 + 1 - core) * 32 + lane
    across = ((1 - x_hi) * 2 + core) * 32 + lane

    def to_partner(k):
        return pltpu.make_async_remote_copy(
            src_ref=prob.at[k, 1 - core], dst_ref=half.at[k],
            send_sem=d_send.at[k], recv_sem=d_recv.at[k], device_id=partner, device_id_type=LOGICAL,
        )

    def to_across(k):
        return pltpu.make_async_remote_copy(
            src_ref=mine.at[k, 1 - x_hi], dst_ref=part.at[k],
            send_sem=m_send.at[k], recv_sem=m_recv.at[k], device_id=across, device_id_type=LOGICAL,
        )

    def direct(other):
        c = lax.rem(core + other, 2)
        h = lax.rem(x_hi + other // 2, 2)
        return pltpu.make_async_remote_copy(
            src_ref=prob.at[3, c, h], dst_ref=last.at[other - 1],
            send_sem=l_send.at[other - 1], recv_sem=l_recv.at[other - 1],
            device_id=(h * 2 + c) * 32 + lane, device_id_type=LOGICAL,
        )

    def add_partner(k):
        to_partner(k).wait_recv()
        for h in range(2):
            mine[k, h] = prob[k, core, h] + half[k, h]
        to_across(k).start()

    for k in range(4):
        if k == 0:
            returned(0, 0, r_recv).wait()
        if k % (4 // STEPS) == 0:
            returned(1, k // (4 // STEPS), r_recv).wait()
        blocks = []
        for q in range(2):
            sign = 1.0 - 2.0 * q
            blocks += left(a2[0, 0, k] + sign * a2[0, 1, k], a2[1, 0, k] + sign * a2[1, 1, k])
        got = right(jnp.concatenate(blocks, axis=0))
        for q in range(2):
            re, im = got[q * 256 : q * 256 + 128], got[q * 256 + 128 : q * 256 + 256]
            out_ref[0, q, k] = re
            out_ref[1, q, k] = im
            chance = re * re + im * im
            for h in range(2):
                for c in range(2):
                    at = (h * 2 + c) * 32
                    prob[k, c, h, q] = chance[at : at + 32]
        if k < 3:
            to_partner(k).start()
        else:
            for other in (2, 3, 1):
                direct(other).start()
        if k:
            add_partner(k - 1)
    for k in range(3):
        to_across(k).wait_recv()
        for q in range(2):
            marg_ref[q, k] = (mine[k, x_hi, q] + part[k, q]) * 0.25
    for other in (1, 2, 3):
        direct(other).wait_recv()
    for q in range(2):
        marg_ref[q, 3] = ((prob[3, core, x_hi, q] + last[0, q]) + (last[1, q] + last[2, q])) * 0.25
    for k in range(3):
        to_partner(k).wait_send()
        to_across(k).wait_send()
        direct(k + 1).wait_send()
    for q in range(2):
        energies_done(q, e_send).wait()
        pltpu.make_async_copy(bt.at[q, :, pl.ds(0, 508)], bt.at[q, :, pl.ds(0, 508)], t_send.at[q]).wait()
        for step in range(STEPS if q else 1):
            returned(q, step, r_send).wait()


def leave(values_ref, marginal_ref, out_ref, marg_ref, sem):
    copies = [pltpu.make_async_copy(values_ref.at[i], out_ref.at[i], sem.at[i]) for i in range(2)]
    copies.append(pltpu.make_async_copy(marginal_ref, marg_ref, sem.at[2]))
    for copy in copies:
        copy.start()
    for copy in copies:
        copy.wait()


def shards(amplitudes, energies, angles):
    f32, bf16 = jnp.float32, jnp.bfloat16
    dma = pltpu.SemaphoreType.DMA
    out, marginal = pl.pallas_call(
        kernel,
        name="walsh",
        out_shape=(
            jax.ShapeDtypeStruct((2, 2, 4, 128, 128), f32),
            jax.ShapeDtypeStruct((2, 4, 32, 128), f32),
        ),
        in_specs=[
            pl.BlockSpec(memory_space=pltpu.HBM),
            pl.BlockSpec(memory_space=pltpu.HBM),
            pl.BlockSpec(memory_space=pltpu.HBM),
        ],
        out_specs=(pl.BlockSpec(memory_space=pltpu.VMEM), pl.BlockSpec(memory_space=pltpu.VMEM)),
        scratch_shapes=[
            pltpu.VMEM((2, 2, 4, 128, 128), f32),
            pltpu.VMEM((2, 4, 128, 128), f32),
            pltpu.VMEM((2, 128), f32),
            pltpu.VMEM((2, 512, 128), f32),
            pltpu.VMEM((2, 2, 512, 128), f32),
            pltpu.VMEM((2, 2, 512, 128), f32),
            pltpu.VMEM((2, 2, 512, 128), f32),
            pltpu.VMEM((2, 2, 4, 128, 128), f32),
            pltpu.VMEM((4, 2, 2, 2, 32, 128), f32),
            pltpu.VMEM((3, 2, 2, 32, 128), f32),
            pltpu.VMEM((3, 2, 2, 32, 128), f32),
            pltpu.VMEM((3, 2, 32, 128), f32),
            pltpu.VMEM((3, 2, 32, 128), f32),
            pltpu.VMEM((128, 256), bf16),
            pltpu.VMEM((256, 128), bf16),
            dma((3,)), dma((2,)), dma((2,)), dma((2,)), dma((2,)), dma((2, 4)), dma((2, 4)),
            dma((3,)), dma((3,)), dma((3,)), dma((3,)), dma((3,)), dma((3,)),
        ],
        compiler_params=pltpu.CompilerParams(
            collective_id=0, has_side_effects=True, vmem_limit_bytes=48 << 20
        ),
    )(
        pltpu.with_memory_space_constraint(amplitudes.reshape(2, 2, 4, 128, 128), pltpu.HBM),
        pltpu.with_memory_space_constraint(energies.reshape(2, 4, 128, 128), pltpu.HBM),
        pltpu.with_memory_space_constraint(angles, pltpu.HBM),
    )
    out, marginal = pl.pallas_call(
        leave,
        name="leave",
        out_shape=(
            jax.ShapeDtypeStruct(out.shape, f32),
            jax.ShapeDtypeStruct(marginal.shape, f32),
        ),
        in_specs=[pl.BlockSpec(memory_space=pltpu.VMEM)] * 2,
        out_specs=[pl.BlockSpec(memory_space=pltpu.HBM)] * 2,
        scratch_shapes=[dma((3,))],
        compiler_params=pltpu.CompilerParams(vmem_limit_bytes=8 << 20),
    )(
        pltpu.with_memory_space_constraint(out, pltpu.VMEM),
        pltpu.with_memory_space_constraint(marginal, pltpu.VMEM),
    )
    return out.reshape(2, 8, 128, 128), marginal.reshape(8, 32, 128)


def solution(mesh):
    return jax.shard_map(
        shards,
        mesh=mesh,
        in_specs=(P(None, ("bank", "lane"), None, None), P(("bank", "lane"), None, None), P()),
        out_specs=(P(None, ("bank", "lane"), None, None), P("lane", "bank", None)),
        check_vma=False,
    )
```

```python
import collections
import itertools

import jax
import jax.numpy as jnp
from jax import lax
from jax.experimental import pallas as pl
from jax.experimental.pallas import tpu as pltpu
from jax.sharding import PartitionSpec as P

LOGICAL = pl.DeviceIdType.LOGICAL
LAYER_SCALE = 2.0**-12
SIN = (
    1.0,
    -0.1666666716337204,
    0.00833333283662796,
    -0.00019841179891955107,
    2.755283276201226e-06,
    -2.493705153483461e-08,
    1.458471399207184e-10,
)
COS = (
    1.0,
    -0.5,
    0.0416666679084301,
    -0.0013888886896893382,
    2.4801460313028656e-05,
    -2.75526161885864e-07,
    2.0779600262699205e-09,
    -1.0417342335977686e-11,
)


def polynomial(coefficients, u):
    total = jnp.full_like(u, coefficients[-1] * LAYER_SCALE)
    for c in coefficients[-2::-1]:
        total = total * u + c * LAYER_SCALE
    return total


def scaled_cos_sin(turn):
    u = turn * turn
    return polynomial(COS, u), polynomial(SIN, u) * turn


def halves(x):
    high = x.astype(jnp.bfloat16)
    low = (x - high.astype(jnp.float32)).astype(jnp.bfloat16)
    return high, low


def position():
    b, l = lax.axis_index("bank"), lax.axis_index("lane")
    x = lax.div(b, 2) * 2 + lax.rem(l, 2)
    return x, lax.rem(lax.div(l, 2), 4), lax.div(l, 8), lax.rem(b, 2)


def hops(d):
    return min(d, 4 - d)


def peer_offsets():
    todo = [o for o in itertools.product(range(4), range(4), range(4), range(2)) if any(o)]
    links = lambda ax, d: [(ax, 1)] if d == 1 else [(ax, -1)] if d == 3 else [(ax, 1), (ax, -1)]
    load, order = collections.Counter(), []
    while todo:
        far = max(sum(map(hops, o[:3])) for o in todo)

        def cost(o):
            uses = [links(ax, d) for ax, d in enumerate(o[:3]) if d]
            return sum(sum(load[u] for u in use) / len(use) for use in uses)

        best = min((o for o in todo if sum(map(hops, o[:3])) == far), key=cost)
        todo.remove(best)
        order.append(best)
        for ax, d in enumerate(best[:3]):
            if d:
                for use in links(ax, d):
                    load[use] += hops(d) / len(links(ax, d))
    return order


OFFSETS = peer_offsets()


def peers():
    x, y, z, core = position()
    xs = {}
    for dx, dc in itertools.product(range(4), range(2)):
        xx, cc = lax.rem(x + dx, 4), lax.rem(core + dc, 2)
        xs[dx, dc] = (lax.div(xx, 2) * 2 + cc) * 32 + lax.rem(xx, 2)
    ys = [lax.rem(y + d, 4) * 2 for d in range(4)]
    zs = [lax.rem(z + d, 4) * 8 for d in range(4)]
    return xs, ys, zs


def for_peers(numbers, visit):
    xs, ys, zs = numbers
    for dx, dy, dz, dc in OFFSETS:
        visit(xs[dx, dc] + (ys[dy] + zs[dz]))


ORDER = [(1, 1), (1, 0), (0, 1), (0, 0)]


def leading(bank, step):
    dh, dc = ORDER[step]
    return lax.rem(lax.div(bank, 2) + dh, 2) * 2 + lax.rem(lax.rem(bank, 2) + dc, 2)


STARTS = [0, 1, 2]


def width_of(step):
    return 1 if step + 1 in STARTS or step == 3 else 2


def first_of_pair(bank, step):
    return lax.rem(lax.div(bank, 2) + ORDER[step][0], 2) * 2


def kernel(
    amp_ref, en_ref, angle_ref, out_ref, marg_ref,
    a_parts, e_parts, angles, eb, bt, cs, b2, a2, prob, half, mine, part,
    wide, tall, load_sem, e_send, e_recv, t_send, t_recv, r_send, r_recv,
    d_send, d_recv, m_send, m_recv,
):
    bank, lane = lax.axis_index("bank"), lax.axis_index("lane")
    me = bank * 32 + lane
    core, x_hi = lax.rem(bank, 2), lax.div(bank, 2)

    numbers = peers()
    barrier = pltpu.get_barrier_semaphore()
    a, e = a_parts.reshape(2, 2, 4, 128, 128), e_parts.reshape(2, 4, 128, 128)
    loads = []
    for t in range(4):
        rows = pl.ds(t * 32, 32)
        loads.append(pltpu.make_async_copy(en_ref.at[:, :, rows, :], e_parts.at[:, t], load_sem.at[0, t]))
        loads.append(pltpu.make_async_copy(amp_ref.at[:, :, :, rows, :], a_parts.at[:, :, t], load_sem.at[1, t]))
    load_angles = pltpu.make_async_copy(angle_ref, angles, load_sem.at[2, 0])
    load_angles.start()
    for load in loads:
        load.start()
    for_peers(numbers, lambda d: pl.semaphore_signal(barrier, inc=1, device_id=d, device_id_type=LOGICAL))

    both = lax.broadcasted_iota(jnp.int32, (128, 256), 0) & (lax.broadcasted_iota(jnp.int32, (128, 256), 1) % 128)
    for s in (4, 2, 1):
        both = both ^ (both >> s)
    wide[...] = (1 - 2 * (both & 1)).astype(jnp.float32).astype(jnp.bfloat16)
    both = lax.broadcasted_iota(jnp.int32, (256, 128), 1) & (lax.broadcasted_iota(jnp.int32, (256, 128), 0) % 128)
    for s in (4, 2, 1):
        both = both ^ (both >> s)
    tall[...] = (1 - 2 * (both & 1)).astype(jnp.float32).astype(jnp.bfloat16)


    def send_energies(q):
        for_peers(
            numbers,
            lambda d: pltpu.make_async_remote_copy(
                src_ref=e.at[q, :, d, :],
                dst_ref=eb.at[q, pl.ds(pl.multiple_of(me * 4, 4), 4), :],
                send_sem=e_send.at[q], recv_sem=e_recv.at[q], device_id=d, device_id_type=LOGICAL,
            ).start()
        )

    def energies_done(q, sem):
        rows = eb.at[q, pl.ds(0, 508)]
        return pltpu.make_async_copy(rows, rows, sem.at[q])

    load_angles.wait()
    for load in loads:
        load.wait()

    def left(re, im):
        rh, rl = halves(re)
        ih, il = halves(im)
        rhs = jnp.concatenate(
            [jnp.concatenate([rh, ih], axis=1), jnp.concatenate([rl, il], axis=1)], axis=0
        )
        got = jnp.dot(wide[...], rhs, preferred_element_type=jnp.float32)
        return got[:, :128], got[:, 128:]

    def right(block):
        return jnp.dot(
            jnp.concatenate(halves(block), axis=1), tall[...], preferred_element_type=jnp.float32
        )

    angle = angles[...]

    def first(k, carry):
        blocks = []
        for q in range(2):
            c, s = scaled_cos_sin(e[q, k] * angle[0:1, :])
            re, im = a[0, q, k], a[1, q, k]
            blocks += [re * c + im * s, im * c - re * s]
        got = right(jnp.concatenate(blocks, axis=0))
        got = [got[i * 128 : (i + 1) * 128] for i in range(4)]
        for q in range(2):
            sign = 1.0 - 2.0 * q
            re, im = left(got[0] + sign * got[2], got[1] + sign * got[3])
            a[0, q, k] = re
            a[1, q, k] = im
        return carry

    lax.fori_loop(0, 4, first, 0)
    pl.semaphore_wait(barrier, 127)

    for q in range(2):
        send_energies(q)
        for_peers(
            numbers,
            lambda d: pltpu.make_async_remote_copy(
                src_ref=a.at[:, q, :, d, :],
                dst_ref=bt.at[q, :, pl.ds(pl.multiple_of(me * 4, 4), 4), :],
                send_sem=t_send.at[q], recv_sem=t_recv.at[q], device_id=d, device_id_type=LOGICAL,
            ).start()
        )
    for q in range(2):
        for k in range(4):
            eb[q, pl.ds(me * 4 + k, 1), :] = e[q, k, pl.ds(me, 1), :]
            for i in range(2):
                bt[q, i, pl.ds(me * 4 + k, 1), :] = a[i, q, k, pl.ds(me, 1), :]

    def returned(q, step, sem):
        if q == 0:
            rows = a2.at[:, 0, :, pl.ds(0, 127)]
        elif width_of(step) == 1:
            rows = a2.at[:, 1, leading(bank, step), pl.ds(0, 127)]
        else:
            rows = a2.at[:, 1, pl.ds(first_of_pair(bank, step), 2), pl.ds(0, 127)]
        return pltpu.make_async_copy(rows, rows, sem.at[q, step])

    for q in range(2):
        energies_done(q, e_recv).wait()

        def turns(r, carry):
            rows = pl.ds(pl.multiple_of(r * 64, 64), 64)
            c, s = scaled_cos_sin(eb[q, rows, :] * angle[1:2, :])
            cs[q, 0, rows, :] = c
            cs[q, 1, rows, :] = s
            return carry

        lax.fori_loop(0, 8, turns, 0)
        pltpu.make_async_copy(bt.at[q, :, pl.ds(0, 508)], bt.at[q, :, pl.ds(0, 508)], t_recv.at[q]).wait()

        def over_rows(src, dst):
            for r in range(4):
                rows = slice(r * 128, (r + 1) * 128)
                re, im = left(src[q, 0, rows, :], src[q, 1, rows, :])
                dst[q, 0, rows, :] = re
                dst[q, 1, rows, :] = im

        over_rows(bt, b2)

        def middle(r, carry):
            def four(v):
                s, d, t, u = v[0] + v[1], v[0] - v[1], v[2] + v[3], v[2] - v[3]
                return [s + t, d + u, s - t, d - u]

            rows = [pl.ds(pl.multiple_of(r * 8, 8) + 128 * h, 8) for h in range(4)]
            re = four([b2[q, 0, w, :] for w in rows])
            im = four([b2[q, 1, w, :] for w in rows])
            cc = [cs[q, 0, w, :] for w in rows]
            ss = [cs[q, 1, w, :] for w in rows]
            re, im = (
                four([x * c + y * s for x, y, c, s in zip(re, im, cc, ss)]),
                four([y * c - x * s for x, y, c, s in zip(re, im, cc, ss)]),
            )
            for h in range(4):
                bt[q, 0, rows[h], :] = re[h]
                bt[q, 1, rows[h], :] = im[h]
            return carry

        lax.fori_loop(0, 16, middle, 0, unroll=4)
        over_rows(bt, b2)

        if q == 0:
            for_peers(
                numbers,
                lambda d: pltpu.make_async_remote_copy(
                    src_ref=b2.at[0, :, pl.ds(d * 4, 4), :], dst_ref=a2.at[:, 0, :, me, :],
                    send_sem=r_send.at[0, 0], recv_sem=r_recv.at[0, 0], device_id=d, device_id_type=LOGICAL,
                ).start()
            )
        else:
            for step in STARTS:
                wide_step = width_of(step)
                banks = {
                    k: leading(lax.div(v, 32), step) if wide_step == 1 else first_of_pair(lax.div(v, 32), step)
                    for k, v in numbers[0].items()
                }
                xs, ys, zs = numbers
                for dx, dy, dz, dc in OFFSETS:
                    d, t = xs[dx, dc] + (ys[dy] + zs[dz]), banks[dx, dc]
                    pltpu.make_async_remote_copy(
                        src_ref=b2.at[1, :, pl.ds(d * 4 + t, wide_step), :], dst_ref=a2.at[:, 1, pl.ds(t, wide_step), me, :],
                        send_sem=r_send.at[1, step], recv_sem=r_recv.at[1, step], device_id=d, device_id_type=LOGICAL,
                    ).start()
        for k in range(4):
            for i in range(2):
                a2[i, q, k, pl.ds(me, 1), :] = b2[q, i, pl.ds(me * 4 + k, 1), :]

    partner = (x_hi * 2 + 1 - core) * 32 + lane
    across = ((1 - x_hi) * 2 + core) * 32 + lane

    def to_partner(n):
        return pltpu.make_async_remote_copy(
            src_ref=prob.at[2 * n], dst_ref=half.at[n],
            send_sem=d_send.at[n], recv_sem=d_recv.at[n], device_id=partner, device_id_type=LOGICAL,
        )

    def to_across(q):
        return pltpu.make_async_remote_copy(
            src_ref=mine.at[q], dst_ref=part.at[q],
            send_sem=m_send.at[q], recv_sem=m_recv.at[q], device_id=across, device_id_type=LOGICAL,
        )

    returned(0, 0, r_recv).wait()
    for step in range(4):
        t = leading(bank, step)
        rows = pl.ds(pl.multiple_of(t * 32, 32), 32)
        if step in STARTS:
            returned(1, step, r_recv).wait()
        for q in range(2):
            sign = 1.0 - 2.0 * q
            re, im = left(a2[0, 0, t] + sign * a2[0, 1, t], a2[1, 0, t] + sign * a2[1, 1, t])
            got = right(jnp.concatenate([re, im], axis=0))
            re, im = got[:128], got[128:]
            chance = re * re + im * im
            for k in range(4):
                at = slice(k * 32, (k + 1) * 32)
                out_ref[0, q, k, rows, :] = re[at]
                out_ref[1, q, k, rows, :] = im[at]
                prob[step, q, k] = chance[at]
            if step == 1:
                if q == 0:
                    to_partner(0).wait_recv()
                mine[q] = prob[1, q] + half[0, q]
                to_across(q).start()
        if step in (0, 2):
            to_partner(step // 2).start()
    to_partner(1).wait_recv()
    for q in range(2):
        to_across(q).wait_recv()
        marg_ref[q] = ((prob[3, q] + half[1, q]) + part[q]) * 0.25
    for q in range(2):
        to_partner(q).wait_send()
        to_across(q).wait_send()
    returned(0, 0, r_send).wait()
    for step in STARTS:
        returned(1, step, r_send).wait()
    for q in range(2):
        energies_done(q, e_send).wait()
        pltpu.make_async_copy(bt.at[q, :, pl.ds(0, 508)], bt.at[q, :, pl.ds(0, 508)], t_send.at[q]).wait()


def leave(values_ref, marginal_ref, out_ref, marg_ref, sem):
    copies = [pltpu.make_async_copy(values_ref.at[i], out_ref.at[i], sem.at[i]) for i in range(2)]
    copies.append(pltpu.make_async_copy(marginal_ref, marg_ref, sem.at[2]))
    for copy in copies:
        copy.start()
    for copy in copies:
        copy.wait()


def shards(amplitudes, energies, angles):
    f32, bf16 = jnp.float32, jnp.bfloat16
    dma = pltpu.SemaphoreType.DMA
    out, marginal = pl.pallas_call(
        kernel,
        name="walsh",
        out_shape=(
            jax.ShapeDtypeStruct((2, 2, 4, 128, 128), f32),
            jax.ShapeDtypeStruct((2, 4, 32, 128), f32),
        ),
        in_specs=[
            pl.BlockSpec(memory_space=pltpu.HBM),
            pl.BlockSpec(memory_space=pltpu.HBM),
            pl.BlockSpec(memory_space=pltpu.HBM),
        ],
        out_specs=(pl.BlockSpec(memory_space=pltpu.VMEM), pl.BlockSpec(memory_space=pltpu.VMEM)),
        scratch_shapes=[
            pltpu.VMEM((2, 2, 4, 4, 32, 128), f32),
            pltpu.VMEM((2, 4, 4, 32, 128), f32),
            pltpu.VMEM((2, 128), f32),
            pltpu.VMEM((2, 512, 128), f32),
            pltpu.VMEM((2, 2, 512, 128), f32),
            pltpu.VMEM((2, 2, 512, 128), f32),
            pltpu.VMEM((2, 2, 512, 128), f32),
            pltpu.VMEM((2, 2, 4, 128, 128), f32),
            pltpu.VMEM((4, 2, 4, 32, 128), f32),
            pltpu.VMEM((2, 2, 4, 32, 128), f32),
            pltpu.VMEM((2, 4, 32, 128), f32),
            pltpu.VMEM((2, 4, 32, 128), f32),
            pltpu.VMEM((128, 256), bf16),
            pltpu.VMEM((256, 128), bf16),
            dma((3, 4)), dma((2,)), dma((2,)), dma((2,)), dma((2,)), dma((2, 4)), dma((2, 4)),
            dma((2,)), dma((2,)), dma((2,)), dma((2,)),
        ],
        compiler_params=pltpu.CompilerParams(
            collective_id=0, has_side_effects=True, vmem_limit_bytes=48 << 20
        ),
    )(
        pltpu.with_memory_space_constraint(amplitudes.reshape(2, 2, 4, 128, 128), pltpu.HBM),
        pltpu.with_memory_space_constraint(energies.reshape(2, 4, 128, 128), pltpu.HBM),
        pltpu.with_memory_space_constraint(angles, pltpu.HBM),
    )
    out, marginal = pl.pallas_call(
        leave,
        name="leave",
        out_shape=(
            jax.ShapeDtypeStruct(out.shape, f32),
            jax.ShapeDtypeStruct(marginal.shape, f32),
        ),
        in_specs=[pl.BlockSpec(memory_space=pltpu.VMEM)] * 2,
        out_specs=[pl.BlockSpec(memory_space=pltpu.HBM)] * 2,
        scratch_shapes=[dma((3,))],
        compiler_params=pltpu.CompilerParams(vmem_limit_bytes=8 << 20),
    )(
        pltpu.with_memory_space_constraint(out, pltpu.VMEM),
        pltpu.with_memory_space_constraint(marginal, pltpu.VMEM),
    )
    return out.reshape(2, 8, 128, 128), marginal.reshape(8, 32, 128)


def solution(mesh):
    return jax.shard_map(
        shards,
        mesh=mesh,
        in_specs=(P(None, ("bank", "lane"), None, None), P(("bank", "lane"), None, None), P()),
        out_specs=(P(None, ("bank", "lane"), None, None), P("lane", "bank", None)),
        check_vma=False,
    )
```

```python
import collections
import itertools

import jax
import jax.numpy as jnp
from jax import lax
from jax.experimental import pallas as pl
from jax.experimental.pallas import tpu as pltpu
from jax.sharding import PartitionSpec as P

LOGICAL = pl.DeviceIdType.LOGICAL
LAYER_SCALE = 2.0**-12
SIN = (
    1.0,
    -0.1666666716337204,
    0.00833333283662796,
    -0.00019841179891955107,
    2.755283276201226e-06,
    -2.493705153483461e-08,
    1.458471399207184e-10,
)
COS = (
    1.0,
    -0.5,
    0.0416666679084301,
    -0.0013888886896893382,
    2.4801460313028656e-05,
    -2.75526161885864e-07,
    2.0779600262699205e-09,
    -1.0417342335977686e-11,
)


def polynomial(coefficients, u):
    total = jnp.full_like(u, coefficients[-1] * LAYER_SCALE)
    for c in coefficients[-2::-1]:
        total = total * u + c * LAYER_SCALE
    return total


def scaled_cos_sin(turn):
    u = turn * turn
    return polynomial(COS, u), polynomial(SIN, u) * turn


def halves(x):
    high = x.astype(jnp.bfloat16)
    low = (x - high.astype(jnp.float32)).astype(jnp.bfloat16)
    return high, low


def position():
    b, l = lax.axis_index("bank"), lax.axis_index("lane")
    x = lax.div(b, 2) * 2 + lax.rem(l, 2)
    return x, lax.rem(lax.div(l, 2), 4), lax.div(l, 8), lax.rem(b, 2)


def hops(d):
    return min(d, 4 - d)


def peer_offsets():
    todo = [o for o in itertools.product(range(4), range(4), range(4), range(2)) if any(o)]
    links = lambda ax, d: [(ax, 1)] if d == 1 else [(ax, -1)] if d == 3 else [(ax, 1), (ax, -1)]
    load, order = collections.Counter(), []
    while todo:
        far = max(sum(map(hops, o[:3])) for o in todo)

        def cost(o):
            uses = [links(ax, d) for ax, d in enumerate(o[:3]) if d]
            return sum(sum(load[u] for u in use) / len(use) for use in uses)

        best = min((o for o in todo if sum(map(hops, o[:3])) == far), key=cost)
        todo.remove(best)
        order.append(best)
        for ax, d in enumerate(best[:3]):
            if d:
                for use in links(ax, d):
                    load[use] += hops(d) / len(links(ax, d))
    return order


OFFSETS = peer_offsets()


def peers():
    x, y, z, core = position()
    xs = {}
    for dx, dc in itertools.product(range(4), range(2)):
        xx, cc = lax.rem(x + dx, 4), lax.rem(core + dc, 2)
        xs[dx, dc] = (lax.div(xx, 2) * 2 + cc) * 32 + lax.rem(xx, 2)
    ys = [lax.rem(y + d, 4) * 2 for d in range(4)]
    zs = [lax.rem(z + d, 4) * 8 for d in range(4)]
    return xs, ys, zs


def for_peers(numbers, visit):
    xs, ys, zs = numbers
    for dx, dy, dz, dc in OFFSETS:
        visit(xs[dx, dc] + (ys[dy] + zs[dz]))


ORDER = [(1, 1), (1, 0), (0, 1), (0, 0)]


def leading(bank, step):
    dh, dc = ORDER[step]
    return lax.rem(lax.div(bank, 2) + dh, 2) * 2 + lax.rem(lax.rem(bank, 2) + dc, 2)


STARTS = [0, 1, 2]


def width_of(step):
    return 1 if step + 1 in STARTS or step == 3 else 2


def first_of_pair(bank, step):
    return lax.rem(lax.div(bank, 2) + ORDER[step][0], 2) * 2


def kernel(
    amp_ref, en_ref, angle_ref, out_ref, marg_ref,
    a_parts, e_parts, angles, eb, bt, cs, b2, a2, prob, half, mine, part,
    wide, tall, load_sem, e_send, e_recv, t_send, t_recv, r_send, r_recv,
    d_send, d_recv, m_send, m_recv,
):
    bank, lane = lax.axis_index("bank"), lax.axis_index("lane")
    me = bank * 32 + lane
    core, x_hi = lax.rem(bank, 2), lax.div(bank, 2)

    numbers = peers()
    barrier = pltpu.get_barrier_semaphore()
    a, e = a_parts.reshape(2, 2, 4, 128, 128), e_parts.reshape(2, 4, 128, 128)
    loads = []
    for t in range(4):
        rows = pl.ds(t * 32, 32)
        loads.append(pltpu.make_async_copy(en_ref.at[:, :, rows, :], e_parts.at[:, t], load_sem.at[0, t]))
        loads.append(pltpu.make_async_copy(amp_ref.at[:, :, :, rows, :], a_parts.at[:, :, t], load_sem.at[1, t]))
    load_angles = pltpu.make_async_copy(angle_ref, angles, load_sem.at[2, 0])
    load_angles.start()
    for load in loads:
        load.start()
    for_peers(numbers, lambda d: pl.semaphore_signal(barrier, inc=1, device_id=d, device_id_type=LOGICAL))

    both = lax.broadcasted_iota(jnp.int32, (128, 256), 0) & (lax.broadcasted_iota(jnp.int32, (128, 256), 1) % 128)
    for s in (4, 2, 1):
        both = both ^ (both >> s)
    wide[...] = (1 - 2 * (both & 1)).astype(jnp.float32).astype(jnp.bfloat16)
    both = lax.broadcasted_iota(jnp.int32, (256, 128), 1) & (lax.broadcasted_iota(jnp.int32, (256, 128), 0) % 128)
    for s in (4, 2, 1):
        both = both ^ (both >> s)
    tall[...] = (1 - 2 * (both & 1)).astype(jnp.float32).astype(jnp.bfloat16)


    def send_energies(q):
        for_peers(
            numbers,
            lambda d: pltpu.make_async_remote_copy(
                src_ref=e.at[q, :, d, :],
                dst_ref=eb.at[q, pl.ds(pl.multiple_of(me * 4, 4), 4), :],
                send_sem=e_send.at[q], recv_sem=e_recv.at[q], device_id=d, device_id_type=LOGICAL,
            ).start()
        )

    def energies_done(q, sem):
        rows = eb.at[q, pl.ds(0, 508)]
        return pltpu.make_async_copy(rows, rows, sem.at[q])

    load_angles.wait()

    def left(re, im):
        rh, rl = halves(re)
        ih, il = halves(im)
        rhs = jnp.concatenate(
            [jnp.concatenate([rh, ih], axis=1), jnp.concatenate([rl, il], axis=1)], axis=0
        )
        got = jnp.dot(wide[...], rhs, preferred_element_type=jnp.float32)
        return got[:, :128], got[:, 128:]

    def right(block):
        return jnp.dot(
            jnp.concatenate(halves(block), axis=1), tall[...], preferred_element_type=jnp.float32
        )

    angle = angles[...]

    def first(k, carry):
        blocks = []
        for q in range(2):
            c, s = scaled_cos_sin(e[q, k] * angle[0:1, :])
            re, im = a[0, q, k], a[1, q, k]
            blocks += [re * c + im * s, im * c - re * s]
        got = right(jnp.concatenate(blocks, axis=0))
        got = [got[i * 128 : (i + 1) * 128] for i in range(4)]
        for q in range(2):
            sign = 1.0 - 2.0 * q
            re, im = left(got[0] + sign * got[2], got[1] + sign * got[3])
            a[0, q, k] = re
            a[1, q, k] = im
        return carry

    for k in range(4):
        loads[2 * k].wait()
        loads[2 * k + 1].wait()
        first(k, 0)
    pl.semaphore_wait(barrier, 127)

    for q in range(2):
        send_energies(q)
        for_peers(
            numbers,
            lambda d: pltpu.make_async_remote_copy(
                src_ref=a.at[:, q, :, d, :],
                dst_ref=bt.at[q, :, pl.ds(pl.multiple_of(me * 4, 4), 4), :],
                send_sem=t_send.at[q], recv_sem=t_recv.at[q], device_id=d, device_id_type=LOGICAL,
            ).start()
        )
    for q in range(2):
        for k in range(4):
            eb[q, pl.ds(me * 4 + k, 1), :] = e[q, k, pl.ds(me, 1), :]
            for i in range(2):
                bt[q, i, pl.ds(me * 4 + k, 1), :] = a[i, q, k, pl.ds(me, 1), :]

    def returned(q, step, sem):
        if q == 0:
            rows = a2.at[:, 0, :, pl.ds(0, 127)]
        elif width_of(step) == 1:
            rows = a2.at[:, 1, leading(bank, step), pl.ds(0, 127)]
        else:
            rows = a2.at[:, 1, pl.ds(first_of_pair(bank, step), 2), pl.ds(0, 127)]
        return pltpu.make_async_copy(rows, rows, sem.at[q, step])

    for q in range(2):
        energies_done(q, e_recv).wait()

        def turns(r, carry):
            rows = pl.ds(pl.multiple_of(r * 64, 64), 64)
            c, s = scaled_cos_sin(eb[q, rows, :] * angle[1:2, :])
            cs[q, 0, rows, :] = c
            cs[q, 1, rows, :] = s
            return carry

        lax.fori_loop(0, 8, turns, 0)
        pltpu.make_async_copy(bt.at[q, :, pl.ds(0, 508)], bt.at[q, :, pl.ds(0, 508)], t_recv.at[q]).wait()

        def over_rows(src, dst):
            for r in range(4):
                rows = slice(r * 128, (r + 1) * 128)
                re, im = left(src[q, 0, rows, :], src[q, 1, rows, :])
                dst[q, 0, rows, :] = re
                dst[q, 1, rows, :] = im

        over_rows(bt, b2)

        def middle(r, carry):
            def four(v):
                s, d, t, u = v[0] + v[1], v[0] - v[1], v[2] + v[3], v[2] - v[3]
                return [s + t, d + u, s - t, d - u]

            rows = [pl.ds(pl.multiple_of(r * 8, 8) + 128 * h, 8) for h in range(4)]
            re = four([b2[q, 0, w, :] for w in rows])
            im = four([b2[q, 1, w, :] for w in rows])
            cc = [cs[q, 0, w, :] for w in rows]
            ss = [cs[q, 1, w, :] for w in rows]
            re, im = (
                four([x * c + y * s for x, y, c, s in zip(re, im, cc, ss)]),
                four([y * c - x * s for x, y, c, s in zip(re, im, cc, ss)]),
            )
            for h in range(4):
                bt[q, 0, rows[h], :] = re[h]
                bt[q, 1, rows[h], :] = im[h]
            return carry

        lax.fori_loop(0, 16, middle, 0, unroll=4)
        over_rows(bt, b2)

        if q == 0:
            for_peers(
                numbers,
                lambda d: pltpu.make_async_remote_copy(
                    src_ref=b2.at[0, :, pl.ds(d * 4, 4), :], dst_ref=a2.at[:, 0, :, me, :],
                    send_sem=r_send.at[0, 0], recv_sem=r_recv.at[0, 0], device_id=d, device_id_type=LOGICAL,
                ).start()
            )
        else:
            for step in STARTS:
                wide_step = width_of(step)
                banks = {
                    k: leading(lax.div(v, 32), step) if wide_step == 1 else first_of_pair(lax.div(v, 32), step)
                    for k, v in numbers[0].items()
                }
                xs, ys, zs = numbers
                for dx, dy, dz, dc in OFFSETS:
                    d, t = xs[dx, dc] + (ys[dy] + zs[dz]), banks[dx, dc]
                    pltpu.make_async_remote_copy(
                        src_ref=b2.at[1, :, pl.ds(d * 4 + t, wide_step), :], dst_ref=a2.at[:, 1, pl.ds(t, wide_step), me, :],
                        send_sem=r_send.at[1, step], recv_sem=r_recv.at[1, step], device_id=d, device_id_type=LOGICAL,
                    ).start()
        for k in range(4):
            for i in range(2):
                a2[i, q, k, pl.ds(me, 1), :] = b2[q, i, pl.ds(me * 4 + k, 1), :]

    partner = (x_hi * 2 + 1 - core) * 32 + lane
    across = ((1 - x_hi) * 2 + core) * 32 + lane

    def to_partner(n, q):
        return pltpu.make_async_remote_copy(
            src_ref=prob.at[2 * n, q], dst_ref=half.at[n, q],
            send_sem=d_send.at[n, q], recv_sem=d_recv.at[n, q], device_id=partner, device_id_type=LOGICAL,
        )

    def to_across(q):
        return pltpu.make_async_remote_copy(
            src_ref=mine.at[q], dst_ref=part.at[q],
            send_sem=m_send.at[q], recv_sem=m_recv.at[q], device_id=across, device_id_type=LOGICAL,
        )

    returned(0, 0, r_recv).wait()
    for step in range(4):
        t = leading(bank, step)
        rows = pl.ds(pl.multiple_of(t * 32, 32), 32)
        if step in STARTS:
            returned(1, step, r_recv).wait()
        for q in range(2):
            sign = 1.0 - 2.0 * q
            re, im = left(a2[0, 0, t] + sign * a2[0, 1, t], a2[1, 0, t] + sign * a2[1, 1, t])
            got = right(jnp.concatenate([re, im], axis=0))
            re, im = got[:128], got[128:]
            chance = re * re + im * im
            for k in range(4):
                at = slice(k * 32, (k + 1) * 32)
                out_ref[0, q, k, rows, :] = re[at]
                out_ref[1, q, k, rows, :] = im[at]
                prob[step, q, k] = chance[at]
            if step in (0, 2):
                to_partner(step // 2, q).start()
            if step == 1:
                to_partner(0, q).wait_recv()
                mine[q] = prob[1, q] + half[0, q]
                to_across(q).start()
    for q in range(2):
        to_partner(1, q).wait_recv()
        to_across(q).wait_recv()
        marg_ref[q] = ((prob[3, q] + half[1, q]) + part[q]) * 0.25
    for q in range(2):
        for n in range(2):
            to_partner(n, q).wait_send()
        to_across(q).wait_send()
    returned(0, 0, r_send).wait()
    for step in STARTS:
        returned(1, step, r_send).wait()
    for q in range(2):
        energies_done(q, e_send).wait()
        pltpu.make_async_copy(bt.at[q, :, pl.ds(0, 508)], bt.at[q, :, pl.ds(0, 508)], t_send.at[q]).wait()


def leave(values_ref, marginal_ref, out_ref, marg_ref, sem):
    copies = [pltpu.make_async_copy(values_ref.at[i], out_ref.at[i], sem.at[i]) for i in range(2)]
    copies.append(pltpu.make_async_copy(marginal_ref, marg_ref, sem.at[2]))
    for copy in copies:
        copy.start()
    for copy in copies:
        copy.wait()


def shards(amplitudes, energies, angles):
    f32, bf16 = jnp.float32, jnp.bfloat16
    dma = pltpu.SemaphoreType.DMA
    out, marginal = pl.pallas_call(
        kernel,
        name="walsh",
        out_shape=(
            jax.ShapeDtypeStruct((2, 2, 4, 128, 128), f32),
            jax.ShapeDtypeStruct((2, 4, 32, 128), f32),
        ),
        in_specs=[
            pl.BlockSpec(memory_space=pltpu.HBM),
            pl.BlockSpec(memory_space=pltpu.HBM),
            pl.BlockSpec(memory_space=pltpu.HBM),
        ],
        out_specs=(pl.BlockSpec(memory_space=pltpu.VMEM), pl.BlockSpec(memory_space=pltpu.VMEM)),
        scratch_shapes=[
            pltpu.VMEM((2, 2, 4, 4, 32, 128), f32),
            pltpu.VMEM((2, 4, 4, 32, 128), f32),
            pltpu.VMEM((2, 128), f32),
            pltpu.VMEM((2, 512, 128), f32),
            pltpu.VMEM((2, 2, 512, 128), f32),
            pltpu.VMEM((2, 2, 512, 128), f32),
            pltpu.VMEM((2, 2, 512, 128), f32),
            pltpu.VMEM((2, 2, 4, 128, 128), f32),
            pltpu.VMEM((4, 2, 4, 32, 128), f32),
            pltpu.VMEM((2, 2, 4, 32, 128), f32),
            pltpu.VMEM((2, 4, 32, 128), f32),
            pltpu.VMEM((2, 4, 32, 128), f32),
            pltpu.VMEM((128, 256), bf16),
            pltpu.VMEM((256, 128), bf16),
            dma((3, 4)), dma((2,)), dma((2,)), dma((2,)), dma((2,)), dma((2, 4)), dma((2, 4)),
            dma((2, 2)), dma((2, 2)), dma((2,)), dma((2,)),
        ],
        compiler_params=pltpu.CompilerParams(
            collective_id=0, has_side_effects=True, vmem_limit_bytes=48 << 20
        ),
    )(
        pltpu.with_memory_space_constraint(amplitudes.reshape(2, 2, 4, 128, 128), pltpu.HBM),
        pltpu.with_memory_space_constraint(energies.reshape(2, 4, 128, 128), pltpu.HBM),
        pltpu.with_memory_space_constraint(angles, pltpu.HBM),
    )
    out, marginal = pl.pallas_call(
        leave,
        name="leave",
        out_shape=(
            jax.ShapeDtypeStruct(out.shape, f32),
            jax.ShapeDtypeStruct(marginal.shape, f32),
        ),
        in_specs=[pl.BlockSpec(memory_space=pltpu.VMEM)] * 2,
        out_specs=[pl.BlockSpec(memory_space=pltpu.HBM)] * 2,
        scratch_shapes=[dma((3,))],
        compiler_params=pltpu.CompilerParams(vmem_limit_bytes=8 << 20),
    )(
        pltpu.with_memory_space_constraint(out, pltpu.VMEM),
        pltpu.with_memory_space_constraint(marginal, pltpu.VMEM),
    )
    return out.reshape(2, 8, 128, 128), marginal.reshape(8, 32, 128)


def solution(mesh):
    return jax.shard_map(
        shards,
        mesh=mesh,
        in_specs=(P(None, ("bank", "lane"), None, None), P(("bank", "lane"), None, None), P()),
        out_specs=(P(None, ("bank", "lane"), None, None), P("lane", "bank", None)),
        check_vma=False,
    )
```

```python
import collections
import itertools

import jax
import jax.numpy as jnp
from jax import lax
from jax.experimental import pallas as pl
from jax.experimental.pallas import tpu as pltpu
from jax.sharding import PartitionSpec as P

LOGICAL = pl.DeviceIdType.LOGICAL
LAYER_SCALE = 2.0**-12
SIN = (
    1.0,
    -0.1666666716337204,
    0.00833333283662796,
    -0.00019841179891955107,
    2.755283276201226e-06,
    -2.493705153483461e-08,
    1.458471399207184e-10,
)
COS = (
    1.0,
    -0.5,
    0.0416666679084301,
    -0.0013888886896893382,
    2.4801460313028656e-05,
    -2.75526161885864e-07,
    2.0779600262699205e-09,
    -1.0417342335977686e-11,
)


def polynomial(coefficients, u):
    total = jnp.full_like(u, coefficients[-1] * LAYER_SCALE)
    for c in coefficients[-2::-1]:
        total = total * u + c * LAYER_SCALE
    return total


def scaled_cos_sin(turn):
    u = turn * turn
    return polynomial(COS, u), polynomial(SIN, u) * turn


def halves(x):
    high = x.astype(jnp.bfloat16)
    low = (x - high.astype(jnp.float32)).astype(jnp.bfloat16)
    return high, low


def position():
    b, l = lax.axis_index("bank"), lax.axis_index("lane")
    x = lax.div(b, 2) * 2 + lax.rem(l, 2)
    return x, lax.rem(lax.div(l, 2), 4), lax.div(l, 8), lax.rem(b, 2)


def hops(d):
    return min(d, 4 - d)


def peer_offsets():
    todo = [o for o in itertools.product(range(4), range(4), range(4), range(2)) if any(o)]
    links = lambda ax, d: [(ax, 1)] if d == 1 else [(ax, -1)] if d == 3 else [(ax, 1), (ax, -1)]
    load, order = collections.Counter(), []
    while todo:
        far = max(sum(map(hops, o[:3])) for o in todo)

        def cost(o):
            uses = [links(ax, d) for ax, d in enumerate(o[:3]) if d]
            return sum(sum(load[u] for u in use) / len(use) for use in uses)

        best = min((o for o in todo if sum(map(hops, o[:3])) == far), key=cost)
        todo.remove(best)
        order.append(best)
        for ax, d in enumerate(best[:3]):
            if d:
                for use in links(ax, d):
                    load[use] += hops(d) / len(links(ax, d))
    return order


OFFSETS = peer_offsets()


def peers():
    x, y, z, core = position()
    xs = {}
    for dx, dc in itertools.product(range(4), range(2)):
        xx, cc = lax.rem(x + dx, 4), lax.rem(core + dc, 2)
        xs[dx, dc] = (lax.div(xx, 2) * 2 + cc) * 32 + lax.rem(xx, 2)
    ys = [lax.rem(y + d, 4) * 2 for d in range(4)]
    zs = [lax.rem(z + d, 4) * 8 for d in range(4)]
    return xs, ys, zs


def for_peers(numbers, visit):
    xs, ys, zs = numbers
    for dx, dy, dz, dc in OFFSETS:
        visit(xs[dx, dc] + (ys[dy] + zs[dz]))


ORDER = [(1, 1), (1, 0), (0, 1), (0, 0)]


def leading(bank, step):
    dh, dc = ORDER[step]
    return lax.rem(lax.div(bank, 2) + dh, 2) * 2 + lax.rem(lax.rem(bank, 2) + dc, 2)


STARTS = [0, 1, 2]


def width_of(step):
    return 1 if step + 1 in STARTS or step == 3 else 2


def first_of_pair(bank, step):
    return lax.rem(lax.div(bank, 2) + ORDER[step][0], 2) * 2


def kernel(
    amp_ref, en_ref, angle_ref, out_ref, marg_ref,
    a_parts, e_parts, angles, eb, bt, cs, b2, a2, prob, half, mine, part,
    wide, tall, load_sem, e_send, e_recv, t_send, t_recv, r_send, r_recv,
    d_send, d_recv, m_send, m_recv,
):
    bank, lane = lax.axis_index("bank"), lax.axis_index("lane")
    me = bank * 32 + lane
    core, x_hi = lax.rem(bank, 2), lax.div(bank, 2)

    numbers = peers()
    barrier = pltpu.get_barrier_semaphore()
    a, e = a_parts.reshape(2, 2, 4, 128, 128), e_parts.reshape(2, 4, 128, 128)
    loads = []
    for t in range(4):
        rows = pl.ds(t * 32, 32)
        loads.append(pltpu.make_async_copy(en_ref.at[:, :, rows, :], e_parts.at[:, t], load_sem.at[0, t]))
        loads.append(pltpu.make_async_copy(amp_ref.at[:, :, :, rows, :], a_parts.at[:, :, t], load_sem.at[1, t]))
    load_angles = pltpu.make_async_copy(angle_ref, angles, load_sem.at[2, 0])
    load_angles.start()
    for load in loads:
        load.start()
    for_peers(numbers, lambda d: pl.semaphore_signal(barrier, inc=1, device_id=d, device_id_type=LOGICAL))

    both = lax.broadcasted_iota(jnp.int32, (128, 256), 0) & (lax.broadcasted_iota(jnp.int32, (128, 256), 1) % 128)
    for s in (4, 2, 1):
        both = both ^ (both >> s)
    wide[...] = (1 - 2 * (both & 1)).astype(jnp.float32).astype(jnp.bfloat16)
    both = lax.broadcasted_iota(jnp.int32, (256, 128), 1) & (lax.broadcasted_iota(jnp.int32, (256, 128), 0) % 128)
    for s in (4, 2, 1):
        both = both ^ (both >> s)
    tall[...] = (1 - 2 * (both & 1)).astype(jnp.float32).astype(jnp.bfloat16)


    def send_energies(q):
        for_peers(
            numbers,
            lambda d: pltpu.make_async_remote_copy(
                src_ref=e.at[q, :, d, :],
                dst_ref=eb.at[q, pl.ds(pl.multiple_of(me * 4, 4), 4), :],
                send_sem=e_send.at[q], recv_sem=e_recv.at[q], device_id=d, device_id_type=LOGICAL,
            ).start()
        )

    def energies_done(q, sem):
        rows = eb.at[q, pl.ds(0, 508)]
        return pltpu.make_async_copy(rows, rows, sem.at[q])

    load_angles.wait()

    def left(re, im):
        rh, rl = halves(re)
        ih, il = halves(im)
        rhs = jnp.concatenate(
            [jnp.concatenate([rh, ih], axis=1), jnp.concatenate([rl, il], axis=1)], axis=0
        )
        got = jnp.dot(wide[...], rhs, preferred_element_type=jnp.float32)
        return got[:, :128], got[:, 128:]

    def right(block):
        return jnp.dot(
            jnp.concatenate(halves(block), axis=1), tall[...], preferred_element_type=jnp.float32
        )

    angle = angles[...]

    def first(k, carry):
        blocks = []
        for q in range(2):
            c, s = scaled_cos_sin(e[q, k] * angle[0:1, :])
            re, im = a[0, q, k], a[1, q, k]
            blocks += [re * c + im * s, im * c - re * s]
        got = right(jnp.concatenate(blocks, axis=0))
        got = [got[i * 128 : (i + 1) * 128] for i in range(4)]
        for q in range(2):
            sign = 1.0 - 2.0 * q
            re, im = left(got[0] + sign * got[2], got[1] + sign * got[3])
            a[0, q, k] = re
            a[1, q, k] = im
        return carry

    for k in range(4):
        loads[2 * k].wait()
        loads[2 * k + 1].wait()
        first(k, 0)
    pl.semaphore_wait(barrier, 127)

    for q in range(2):
        send_energies(q)
        for_peers(
            numbers,
            lambda d: pltpu.make_async_remote_copy(
                src_ref=a.at[:, q, :, d, :],
                dst_ref=bt.at[q, :, pl.ds(pl.multiple_of(me * 4, 4), 4), :],
                send_sem=t_send.at[q], recv_sem=t_recv.at[q], device_id=d, device_id_type=LOGICAL,
            ).start()
        )
    for q in range(2):
        for k in range(4):
            eb[q, pl.ds(me * 4 + k, 1), :] = e[q, k, pl.ds(me, 1), :]
            for i in range(2):
                bt[q, i, pl.ds(me * 4 + k, 1), :] = a[i, q, k, pl.ds(me, 1), :]

    def returned(q, step, sem):
        if q == 0:
            rows = a2.at[:, 0, :, pl.ds(0, 127)]
        elif width_of(step) == 1:
            rows = a2.at[:, 1, leading(bank, step), pl.ds(0, 127)]
        else:
            rows = a2.at[:, 1, pl.ds(first_of_pair(bank, step), 2), pl.ds(0, 127)]
        return pltpu.make_async_copy(rows, rows, sem.at[q, step])

    for q in range(2):
        energies_done(q, e_recv).wait()

        def turns(r, carry):
            rows = pl.ds(pl.multiple_of(r * 64, 64), 64)
            c, s = scaled_cos_sin(eb[q, rows, :] * angle[1:2, :])
            cs[q, 0, rows, :] = c
            cs[q, 1, rows, :] = s
            return carry

        lax.fori_loop(0, 8, turns, 0)
        pltpu.make_async_copy(bt.at[q, :, pl.ds(0, 508)], bt.at[q, :, pl.ds(0, 508)], t_recv.at[q]).wait()

        def over_rows(src, dst):
            for r in range(4):
                rows = slice(r * 128, (r + 1) * 128)
                re, im = left(src[q, 0, rows, :], src[q, 1, rows, :])
                dst[q, 0, rows, :] = re
                dst[q, 1, rows, :] = im

        over_rows(bt, b2)

        def middle(r, carry):
            def four(v):
                s, d, t, u = v[0] + v[1], v[0] - v[1], v[2] + v[3], v[2] - v[3]
                return [s + t, d + u, s - t, d - u]

            rows = [pl.ds(pl.multiple_of(r * 8, 8) + 128 * h, 8) for h in range(4)]
            re = four([b2[q, 0, w, :] for w in rows])
            im = four([b2[q, 1, w, :] for w in rows])
            cc = [cs[q, 0, w, :] for w in rows]
            ss = [cs[q, 1, w, :] for w in rows]
            re, im = (
                four([x * c + y * s for x, y, c, s in zip(re, im, cc, ss)]),
                four([y * c - x * s for x, y, c, s in zip(re, im, cc, ss)]),
            )
            for h in range(4):
                bt[q, 0, rows[h], :] = re[h]
                bt[q, 1, rows[h], :] = im[h]
            return carry

        lax.fori_loop(0, 16, middle, 0, unroll=4)
        over_rows(bt, b2)

        if q == 0:
            for_peers(
                numbers,
                lambda d: pltpu.make_async_remote_copy(
                    src_ref=b2.at[0, :, pl.ds(d * 4, 4), :], dst_ref=a2.at[:, 0, :, me, :],
                    send_sem=r_send.at[0, 0], recv_sem=r_recv.at[0, 0], device_id=d, device_id_type=LOGICAL,
                ).start()
            )
        else:
            for step in STARTS:
                wide_step = width_of(step)
                banks = {
                    k: leading(lax.div(v, 32), step) if wide_step == 1 else first_of_pair(lax.div(v, 32), step)
                    for k, v in numbers[0].items()
                }
                xs, ys, zs = numbers
                for dx, dy, dz, dc in OFFSETS:
                    d, t = xs[dx, dc] + (ys[dy] + zs[dz]), banks[dx, dc]
                    pltpu.make_async_remote_copy(
                        src_ref=b2.at[1, :, pl.ds(d * 4 + t, wide_step), :], dst_ref=a2.at[:, 1, pl.ds(t, wide_step), me, :],
                        send_sem=r_send.at[1, step], recv_sem=r_recv.at[1, step], device_id=d, device_id_type=LOGICAL,
                    ).start()
        for k in range(4):
            for i in range(2):
                a2[i, q, k, pl.ds(me, 1), :] = b2[q, i, pl.ds(me * 4 + k, 1), :]

    partner = (x_hi * 2 + 1 - core) * 32 + lane
    across = ((1 - x_hi) * 2 + core) * 32 + lane

    def to_partner(n, q):
        return pltpu.make_async_remote_copy(
            src_ref=prob.at[2 * n, q], dst_ref=half.at[n, q],
            send_sem=d_send.at[n, q], recv_sem=d_recv.at[n, q], device_id=partner, device_id_type=LOGICAL,
        )

    def to_across(q, pair):
        ks = pl.ds(2 * pair, 2)
        return pltpu.make_async_remote_copy(
            src_ref=mine.at[q, ks], dst_ref=part.at[q, ks],
            send_sem=m_send.at[q, pair], recv_sem=m_recv.at[q, pair], device_id=across, device_id_type=LOGICAL,
        )

    returned(0, 0, r_recv).wait()
    for step in range(4):
        t = leading(bank, step)
        rows = pl.ds(pl.multiple_of(t * 32, 32), 32)
        if step in STARTS:
            returned(1, step, r_recv).wait()
        for q in range(2):
            sign = 1.0 - 2.0 * q
            re, im = left(a2[0, 0, t] + sign * a2[0, 1, t], a2[1, 0, t] + sign * a2[1, 1, t])
            got = right(jnp.concatenate([re, im], axis=0))
            re, im = got[:128], got[128:]
            chance = re * re + im * im
            for k in range(4):
                at = slice(k * 32, (k + 1) * 32)
                out_ref[0, q, k, rows, :] = re[at]
                out_ref[1, q, k, rows, :] = im[at]
                prob[step, q, k] = chance[at]
            if step in (0, 2):
                to_partner(step // 2, q).start()
            if step == 1:
                to_partner(0, q).wait_recv()
                for pair in range(2):
                    ks = slice(2 * pair, 2 * pair + 2)
                    mine[q, ks] = prob[1, q, ks] + half[0, q, ks]
                    to_across(q, pair).start()
    for q in range(2):
        to_partner(1, q).wait_recv()
        for pair in range(2):
            to_across(q, pair).wait_recv()
        marg_ref[q] = ((prob[3, q] + half[1, q]) + part[q]) * 0.25
    for q in range(2):
        for n in range(2):
            to_partner(n, q).wait_send()
        for pair in range(2):
            to_across(q, pair).wait_send()
    returned(0, 0, r_send).wait()
    for step in STARTS:
        returned(1, step, r_send).wait()
    for q in range(2):
        energies_done(q, e_send).wait()
        pltpu.make_async_copy(bt.at[q, :, pl.ds(0, 508)], bt.at[q, :, pl.ds(0, 508)], t_send.at[q]).wait()


def leave(values_ref, marginal_ref, out_ref, marg_ref, sem):
    copies = [pltpu.make_async_copy(values_ref.at[i], out_ref.at[i], sem.at[i]) for i in range(2)]
    copies.append(pltpu.make_async_copy(marginal_ref, marg_ref, sem.at[2]))
    for copy in copies:
        copy.start()
    for copy in copies:
        copy.wait()


def shards(amplitudes, energies, angles):
    f32, bf16 = jnp.float32, jnp.bfloat16
    dma = pltpu.SemaphoreType.DMA
    out, marginal = pl.pallas_call(
        kernel,
        name="walsh",
        out_shape=(
            jax.ShapeDtypeStruct((2, 2, 4, 128, 128), f32),
            jax.ShapeDtypeStruct((2, 4, 32, 128), f32),
        ),
        in_specs=[
            pl.BlockSpec(memory_space=pltpu.HBM),
            pl.BlockSpec(memory_space=pltpu.HBM),
            pl.BlockSpec(memory_space=pltpu.HBM),
        ],
        out_specs=(pl.BlockSpec(memory_space=pltpu.VMEM), pl.BlockSpec(memory_space=pltpu.VMEM)),
        scratch_shapes=[
            pltpu.VMEM((2, 2, 4, 4, 32, 128), f32),
            pltpu.VMEM((2, 4, 4, 32, 128), f32),
            pltpu.VMEM((2, 128), f32),
            pltpu.VMEM((2, 512, 128), f32),
            pltpu.VMEM((2, 2, 512, 128), f32),
            pltpu.VMEM((2, 2, 512, 128), f32),
            pltpu.VMEM((2, 2, 512, 128), f32),
            pltpu.VMEM((2, 2, 4, 128, 128), f32),
            pltpu.VMEM((4, 2, 4, 32, 128), f32),
            pltpu.VMEM((2, 2, 4, 32, 128), f32),
            pltpu.VMEM((2, 4, 32, 128), f32),
            pltpu.VMEM((2, 4, 32, 128), f32),
            pltpu.VMEM((128, 256), bf16),
            pltpu.VMEM((256, 128), bf16),
            dma((3, 4)), dma((2,)), dma((2,)), dma((2,)), dma((2,)), dma((2, 4)), dma((2, 4)),
            dma((2, 2)), dma((2, 2)), dma((2, 2)), dma((2, 2)),
        ],
        compiler_params=pltpu.CompilerParams(
            collective_id=0, has_side_effects=True, vmem_limit_bytes=48 << 20
        ),
    )(
        pltpu.with_memory_space_constraint(amplitudes.reshape(2, 2, 4, 128, 128), pltpu.HBM),
        pltpu.with_memory_space_constraint(energies.reshape(2, 4, 128, 128), pltpu.HBM),
        pltpu.with_memory_space_constraint(angles, pltpu.HBM),
    )
    out, marginal = pl.pallas_call(
        leave,
        name="leave",
        out_shape=(
            jax.ShapeDtypeStruct(out.shape, f32),
            jax.ShapeDtypeStruct(marginal.shape, f32),
        ),
        in_specs=[pl.BlockSpec(memory_space=pltpu.VMEM)] * 2,
        out_specs=[pl.BlockSpec(memory_space=pltpu.HBM)] * 2,
        scratch_shapes=[dma((3,))],
        compiler_params=pltpu.CompilerParams(vmem_limit_bytes=8 << 20),
    )(
        pltpu.with_memory_space_constraint(out, pltpu.VMEM),
        pltpu.with_memory_space_constraint(marginal, pltpu.VMEM),
    )
    return out.reshape(2, 8, 128, 128), marginal.reshape(8, 32, 128)


def solution(mesh):
    return jax.shard_map(
        shards,
        mesh=mesh,
        in_specs=(P(None, ("bank", "lane"), None, None), P(("bank", "lane"), None, None), P()),
        out_specs=(P(None, ("bank", "lane"), None, None), P("lane", "bank", None)),
        check_vma=False,
    )
```
